32 devices in a mesh: dp: 1 (over z), sp: 32 (over y, x, core).
Axes of the slice: x: 4, y: 4, z: 1, core: 2. Of those that a mesh axis runs over, the one named last changes fastest.
The devices are a block of a 4x4x8 slice.
Arguments:
- x: bfloat16 [4, 2048, 512], P('dp', 'sp')
- w_in: bfloat16 [11, 3, 512, 1024], replicated
- w_res: bfloat16 [11, 512, 512], replicated
- w_skip: bfloat16 [11, 512, 512], replicated
Outputs:
- output 1: float32 [4, 2048, 512], P('dp', 'sp')
- output 2: float32 [4, 2048, 512], P('dp', 'sp')
All inputs are finite; a program needn't handle non-finite values.
Results may differ from the reference program's by a relative error of at most 0.00582507.
Values are sent between devices in bfloat16 or wider.
A program may use at most 768 MiB of HBM per device.

```python
import jax
import jax.numpy as jnp

NUM_SEQS = 4
SEQ_LEN = 2048
CHANNELS = 512
SKIP_CH = 512
NUM_LAYERS = 11


def setup_inputs(seed: int = 0, part: int = 0) -> dict:
    root_key = jax.random.key(seed)
    key_x, key_in, key_res, key_skip = jax.random.split(root_key, 4)
    x = jax.random.normal(jax.random.fold_in(key_x, part), (NUM_SEQS, SEQ_LEN, CHANNELS), jnp.float32)
    w_in = jax.random.normal(key_in, (NUM_LAYERS, 3, CHANNELS, 2 * CHANNELS), jnp.float32) * (3 * CHANNELS) ** -0.5
    w_res = jax.random.normal(key_res, (NUM_LAYERS, CHANNELS, CHANNELS), jnp.float32) * (0.5 * CHANNELS ** -0.5)
    w_skip = jax.random.normal(key_skip, (NUM_LAYERS, CHANNELS, SKIP_CH), jnp.float32) * CHANNELS ** -0.5
    return {'x': x.astype(jnp.bfloat16), 'w_in': w_in.astype(jnp.bfloat16), 'w_res': w_res.astype(jnp.bfloat16), 'w_skip': w_skip.astype(jnp.bfloat16)}


def matmul_rows(operand, weight):
    flat = jnp.dot(operand.reshape(-1, operand.shape[-1]), weight, preferred_element_type=jnp.float32)
    return flat.reshape(operand.shape[:-1] + (weight.shape[-1],))


def reference(x, w_in, w_res, w_skip):
    seq_len = x.shape[1]
    n_chan = x.shape[2]
    residual = x.astype(jnp.float32)
    skip_sum = jnp.zeros(x.shape[:2] + (w_skip.shape[2],), jnp.float32)
    for layer in range(NUM_LAYERS):
        dilation = 2 ** layer
        cur_bf = residual.astype(jnp.bfloat16)
        left_tap = jnp.pad(cur_bf[:, :seq_len - dilation], ((0, 0), (dilation, 0), (0, 0)))
        right_tap = jnp.pad(cur_bf[:, dilation:], ((0, 0), (0, dilation), (0, 0)))
        pre_act = matmul_rows(left_tap, w_in[layer, 0]) + matmul_rows(cur_bf, w_in[layer, 1]) + matmul_rows(right_tap, w_in[layer, 2])
        gated = (jnp.tanh(pre_act[..., :n_chan]) * jax.nn.sigmoid(pre_act[..., n_chan:])).astype(jnp.bfloat16)
        residual = residual + matmul_rows(gated, w_res[layer])
        skip_sum = skip_sum + matmul_rows(gated, w_skip[layer])
    return residual, skip_sum
```

```python
import functools

import jax
import jax.numpy as jnp
from jax import lax
from jax.experimental import pallas as pl
from jax.experimental.pallas import tpu as pltpu
from jax.sharding import PartitionSpec as P

MESH = pl.DeviceIdType.MESH
F32, BF16 = jnp.float32, jnp.bfloat16
TILE = 8
HALO = 8
EDGE = 16
COLS = 256


def stack_kernel(n_dev, n_near, x_hbm, win_hbm, wres_hbm, wskip_hbm, h_out, s_out, win, wres, wskip, xv, halo_l, halo_r,
                 near, near_skip, out_blocks, far, far_skip, home_h, home_s, lhs, gate,
                 x_sem, w_sem, halo_send, halo_recv, mid_send, mid_recv, end_send, end_recv):
    me = lax.axis_index('sp')
    n_seq, rows, n_chan = xv.shape
    n_skip = far_skip.shape[1]
    n_layers = win.shape[0]
    far_rows = far_skip.shape[0]
    pad = (far.shape[0] - far_rows) // 2
    n_res = rows // TILE
    last = n_dev - 1

    barrier = pltpu.get_barrier_semaphore()

    @pl.loop(1, n_dev)
    def _(k):
        pl.semaphore_signal(barrier, inc=1, device_id={'sp': lax.rem(me + k, n_dev)}, device_id_type=MESH)

    x_copy = pltpu.make_async_copy(x_hbm, xv, x_sem)
    x_copy.start()

    def weight_copies(layer):
        return [pltpu.make_async_copy(win_hbm.at[layer], win.at[layer], w_sem.at[layer, 0]),
                pltpu.make_async_copy(wres_hbm.at[layer], wres.at[layer], w_sem.at[layer, 1]),
                pltpu.make_async_copy(wskip_hbm.at[layer], wskip.at[layer], w_sem.at[layer, 2])]

    for layer in range(n_layers):
        for copy in weight_copies(layer):
            copy.start()

    zero_edge = jnp.zeros((n_seq, EDGE, n_chan), F32)
    near[:, :EDGE] = zero_edge
    near[:, EDGE + rows:] = zero_edge
    far[:pad] = jnp.zeros((pad, n_chan), F32)
    far[pad + far_rows:] = jnp.zeros((pad, n_chan), F32)

    x_copy.wait()
    pl.semaphore_wait(barrier, n_dev - 1)

    def to_next():
        return pltpu.make_async_remote_copy(src_ref=xv.at[:, pl.ds(rows - HALO, HALO)], dst_ref=halo_l, send_sem=halo_send.at[0],
                                            recv_sem=halo_recv.at[0], device_id={'sp': me + 1}, device_id_type=MESH)

    def to_prev():
        return pltpu.make_async_remote_copy(src_ref=xv.at[:, pl.ds(0, HALO)], dst_ref=halo_r, send_sem=halo_send.at[1],
                                            recv_sem=halo_recv.at[1], device_id={'sp': me - 1}, device_id_type=MESH)

    @pl.when(me < last)
    def _():
        to_next().start()

    @pl.when(me > 0)
    def _():
        to_prev().start()

    near[:, EDGE:EDGE + rows] = xv[...].astype(F32)

    @pl.when(me > 0)
    def _():
        to_next().wait_recv()
        near[:, EDGE - HALO:EDGE] = halo_l[...].astype(F32)

    @pl.when(me < last)
    def _():
        to_prev().wait_recv()
        near[:, EDGE + rows:EDGE + rows + HALO] = halo_r[...].astype(F32)

    def gated_layer(layer, m):
        w = win.at[layer]
        for col in range(0, n_chan, COLS):
            f = jnp.zeros((m, COLS), F32)
            g = jnp.zeros((m, COLS), F32)
            for tap in range(3):
                op = lhs[:m, tap * n_chan:(tap + 1) * n_chan]
                f = f + jnp.dot(op, w[tap, :, col:col + COLS], preferred_element_type=F32)
                g = g + jnp.dot(op, w[tap, :, n_chan + col:n_chan + col + COLS], preferred_element_type=F32)
            gate[:m, col:col + COLS] = (jnp.tanh(f) * (0.5 * jnp.tanh(0.5 * g) + 0.5)).astype(BF16)

    for layer in range(n_near):
        dist = 2 ** layer
        lo, hi = (EDGE - HALO, EDGE + rows + HALO) if layer < n_near - 1 else (EDGE, EDGE + rows)
        size = hi - lo
        m = n_seq * size
        for tap in range(3):
            off = lo + (tap - 1) * dist
            for seq in range(n_seq):
                lhs[seq * size:(seq + 1) * size, tap * n_chan:(tap + 1) * n_chan] = near[seq, off:off + size].astype(BF16)
        for copy in weight_copies(layer):
            copy.wait()
        gated_layer(layer, m)
        for col in range(0, n_chan, COLS):
            res = jnp.dot(gate[:m], wres[layer, :, col:col + COLS], preferred_element_type=F32).reshape(n_seq, size, COLS)
            near[:, lo:hi, col:col + COLS] = near[:, lo:hi, col:col + COLS] + res
        for col in range(0, n_skip, COLS):
            skip = jnp.dot(gate[:m], wskip[layer, :, col:col + COLS], preferred_element_type=F32).reshape(n_seq, size, COLS)
            skip = skip[:, EDGE - lo:EDGE - lo + rows]
            if layer:
                skip = near_skip[:, :, col:col + COLS] + skip
            near_skip[:, :, col:col + COLS] = skip
        if layer < n_near - 1:
            @pl.when(me == 0)
            def _():
                near[:, :EDGE] = zero_edge

            @pl.when(me == last)
            def _():
                near[:, EDGE + rows:] = zero_edge

    for seq in range(n_seq):
        own = near[seq, EDGE:EDGE + rows].reshape(TILE, n_res, n_chan)
        out_blocks[seq * n_res:(seq + 1) * n_res] = jnp.swapaxes(own, 0, 1)

    def mid_copy(dst, src):
        return pltpu.make_async_remote_copy(src_ref=out_blocks.at[dst], dst_ref=far.at[pl.ds(pl.multiple_of(pad + src * TILE, TILE), TILE)],
                                            send_sem=mid_send.at[dst], recv_sem=mid_recv.at[src], device_id={'sp': dst}, device_id_type=MESH)

    @pl.loop(1, n_dev)
    def _(k):
        mid_copy(lax.rem(me + k, n_dev), me).start()

    far[pl.ds(pl.multiple_of(pad + me * TILE, TILE), TILE)] = out_blocks[me]

    @pl.loop(1, n_dev)
    def _(k):
        src = lax.rem(me + n_dev - k, n_dev)
        mid_copy(lax.rem(me + k, n_dev), src).wait_recv()

    for layer in range(n_near, n_layers):
        dist = 2 ** layer // n_res
        for tap in range(3):
            off = pad + (tap - 1) * dist
            lhs[:far_rows, tap * n_chan:(tap + 1) * n_chan] = far[off:off + far_rows].astype(BF16)
        for copy in weight_copies(layer):
            copy.wait()
        gated_layer(layer, far_rows)
        for col in range(0, n_chan, COLS):
            res = jnp.dot(gate[:far_rows], wres[layer, :, col:col + COLS], preferred_element_type=F32)
            far[pad:pad + far_rows, col:col + COLS] = far[pad:pad + far_rows, col:col + COLS] + res
        for col in range(0, n_skip, COLS):
            skip = jnp.dot(gate[:far_rows], wskip[layer, :, col:col + COLS], preferred_element_type=F32)
            if layer > n_near:
                skip = far_skip[:, col:col + COLS] + skip
            far_skip[:, col:col + COLS] = skip

    def end_copy(which, dst, src):
        source = far.at[pl.ds(pl.multiple_of(pad + dst * TILE, TILE), TILE)] if which == 0 else far_skip.at[pl.ds(pl.multiple_of(dst * TILE, TILE), TILE)]
        return pltpu.make_async_remote_copy(src_ref=source, dst_ref=(home_h, home_s)[which].at[src],
                                            send_sem=end_send.at[which, dst], recv_sem=end_recv.at[which, src], device_id={'sp': dst}, device_id_type=MESH)

    for which in range(2):
        @pl.loop(1, n_dev)
        def _(k):
            end_copy(which, lax.rem(me + k, n_dev), me).start()

    home_h[me] = far[pl.ds(pl.multiple_of(pad + me * TILE, TILE), TILE)]
    home_s[me] = far_skip[pl.ds(pl.multiple_of(me * TILE, TILE), TILE)]

    for which in range(2):
        @pl.loop(1, n_dev)
        def _(k):
            end_copy(which, lax.rem(me + k, n_dev), lax.rem(me + n_dev - k, n_dev)).wait_recv()

    for seq in range(n_seq):
        blocks = slice(seq * n_res, (seq + 1) * n_res)
        h_out[seq] = jnp.swapaxes(home_h[blocks], 0, 1).reshape(rows, n_chan)
        s_out[seq] = jnp.swapaxes(home_s[blocks], 0, 1).reshape(rows, n_skip) + near_skip[seq]

    @pl.when(me < last)
    def _():
        to_next().wait_send()

    @pl.when(me > 0)
    def _():
        to_prev().wait_send()

    @pl.loop(1, n_dev)
    def _(k):
        dst = lax.rem(me + k, n_dev)
        mid_copy(dst, me).wait_send()
        end_copy(0, dst, me).wait_send()
        end_copy(1, dst, me).wait_send()


def solution(mesh):
    n_dev = mesh.shape['sp']
    act_spec = P('dp', 'sp', None)

    def local_stack(x, w_in, w_res, w_skip):
        n_seq, rows, n_chan = x.shape
        n_layers, n_skip = w_in.shape[0], w_skip.shape[2]
        n_res = n_dev // n_seq
        n_near = n_res.bit_length() - 1
        far_rows = n_dev * rows // n_res
        pad = 2 ** (n_layers - 1) // n_res
        any_spec = pl.BlockSpec(memory_space=pl.ANY)
        vmem = pl.BlockSpec(memory_space=pltpu.VMEM)
        m_max = n_seq * (rows + 2 * HALO)
        dma = pltpu.SemaphoreType.DMA
        return pl.pallas_call(
            functools.partial(stack_kernel, n_dev, n_near),
            out_shape=(jax.ShapeDtypeStruct((n_seq, rows, n_chan), F32), jax.ShapeDtypeStruct((n_seq, rows, n_skip), F32)),
            in_specs=[any_spec] * 4,
            out_specs=(vmem, vmem),
            scratch_shapes=[
                pltpu.VMEM(w_in.shape, BF16), pltpu.VMEM(w_res.shape, BF16), pltpu.VMEM(w_skip.shape, BF16),
                pltpu.VMEM(x.shape, BF16), pltpu.VMEM((n_seq, HALO, n_chan), BF16), pltpu.VMEM((n_seq, HALO, n_chan), BF16),
                pltpu.VMEM((n_seq, rows + 2 * EDGE, n_chan), F32), pltpu.VMEM((n_seq, rows, n_skip), F32),
                pltpu.VMEM((n_dev, TILE, n_chan), F32),
                pltpu.VMEM((far_rows + 2 * pad, n_chan), F32), pltpu.VMEM((far_rows, n_skip), F32),
                pltpu.VMEM((n_dev, TILE, n_chan), F32), pltpu.VMEM((n_dev, TILE, n_skip), F32),
                pltpu.VMEM((m_max, 3 * n_chan), BF16), pltpu.VMEM((m_max, n_chan), BF16),
                dma, dma((n_layers, 3)), dma((2,)), dma((2,)), dma((n_dev,)), dma((n_dev,)), dma((2, n_dev)), dma((2, n_dev)),
            ],
            compiler_params=pltpu.CompilerParams(collective_id=0, has_side_effects=True, vmem_limit_bytes=63 * 2 ** 20),
            name='dilated_stack',
        )(x, w_in, w_res, w_skip)

    return jax.shard_map(local_stack, mesh=mesh, in_specs=(act_spec, P(), P(), P()), out_specs=(act_spec, act_spec), check_vma=False)
```

```python
import functools

import jax
import jax.numpy as jnp
from jax import lax
from jax.experimental import pallas as pl
from jax.experimental.pallas import tpu as pltpu
from jax.sharding import PartitionSpec as P

MESH = pl.DeviceIdType.MESH
F32, BF16 = jnp.float32, jnp.bfloat16
TILE = 8
HALO = 8
EDGE = 16
COLS = 256


def stack_kernel(n_dev, n_near, x_hbm, win_hbm, wres_hbm, wskip_hbm, home_h, home_s, skip_out, win, wres, wskip, xv, halo_l, halo_r,
                 near, near_skip, out_blocks, far, far_skip, lhs, gate, near_gate,
                 x_sem, own_sem, w_sem, halo_send, halo_recv, mid_send, mid_recv, end_send, end_recv):
    me = lax.axis_index('sp')
    n_seq, rows, n_chan = xv.shape
    n_skip = far_skip.shape[1]
    n_layers = win.shape[0]
    far_rows = far_skip.shape[0]
    pad = (far.shape[0] - far_rows) // 2
    n_res = rows // TILE
    last = n_dev - 1

    barrier = pltpu.get_barrier_semaphore()

    @pl.loop(1, n_dev)
    def _(k):
        pl.semaphore_signal(barrier, inc=1, device_id={'sp': lax.rem(me + k, n_dev)}, device_id_type=MESH)

    x_copy = pltpu.make_async_copy(x_hbm, xv, x_sem)
    x_copy.start()

    def weight_copies(layer):
        return [pltpu.make_async_copy(win_hbm.at[layer], win.at[layer], w_sem.at[layer, 0]),
                pltpu.make_async_copy(wres_hbm.at[layer], wres.at[layer], w_sem.at[layer, 1]),
                pltpu.make_async_copy(wskip_hbm.at[layer], wskip.at[layer], w_sem.at[layer, 2])]

    zero_edge = jnp.zeros((n_seq, EDGE, n_chan), F32)
    near[:, :EDGE] = zero_edge
    near[:, EDGE + rows:] = zero_edge
    far[:pad] = jnp.zeros((pad, n_chan), F32)
    far[pad + far_rows:] = jnp.zeros((pad, n_chan), F32)

    x_copy.wait()
    for layer in range(n_near):
        for copy in weight_copies(layer):
            copy.start()
    pl.semaphore_wait(barrier, n_dev - 1)

    def to_next():
        return pltpu.make_async_remote_copy(src_ref=xv.at[:, pl.ds(rows - HALO, HALO)], dst_ref=halo_l, send_sem=halo_send.at[0],
                                            recv_sem=halo_recv.at[0], device_id={'sp': me + 1}, device_id_type=MESH)

    def to_prev():
        return pltpu.make_async_remote_copy(src_ref=xv.at[:, pl.ds(0, HALO)], dst_ref=halo_r, send_sem=halo_send.at[1],
                                            recv_sem=halo_recv.at[1], device_id={'sp': me - 1}, device_id_type=MESH)

    @pl.when(me < last)
    def _():
        to_next().start()

    @pl.when(me > 0)
    def _():
        to_prev().start()

    near[:, EDGE:EDGE + rows] = xv[...].astype(F32)

    @pl.when(me > 0)
    def _():
        to_next().wait_recv()
        near[:, EDGE - HALO:EDGE] = halo_l[...].astype(F32)

    @pl.when(me < last)
    def _():
        to_prev().wait_recv()
        near[:, EDGE + rows:EDGE + rows + HALO] = halo_r[...].astype(F32)

    def gated_layer(layer, m):
        w = win.at[layer]
        for col in range(0, n_chan, COLS):
            f = jnp.zeros((m, COLS), F32)
            g = jnp.zeros((m, COLS), F32)
            for tap in range(3):
                op = lhs[:m, tap * n_chan:(tap + 1) * n_chan]
                f = f + jnp.dot(op, w[tap, :, col:col + COLS], preferred_element_type=F32)
                g = g + jnp.dot(op, w[tap, :, n_chan + col:n_chan + col + COLS], preferred_element_type=F32)
            gate[:m, col:col + COLS] = (jnp.tanh(f) * (0.5 * jnp.tanh(0.5 * g) + 0.5)).astype(BF16)

    for layer in range(n_near):
        dist = 2 ** layer
        lo, hi = (EDGE - HALO, EDGE + rows + HALO) if layer < n_near - 1 else (EDGE, EDGE + rows)
        size = hi - lo
        m = n_seq * size
        for tap in range(3):
            off = lo + (tap - 1) * dist
            for seq in range(n_seq):
                lhs[seq * size:(seq + 1) * size, tap * n_chan:(tap + 1) * n_chan] = near[seq, off:off + size].astype(BF16)
        for copy in weight_copies(layer):
            copy.wait()
        if layer == n_near - 1:
            for later in range(n_near, n_layers):
                for copy in weight_copies(later):
                    copy.start()
        gated_layer(layer, m)
        for seq in range(n_seq):
            begin = seq * size + EDGE - lo
            near_gate[seq * rows:(seq + 1) * rows, layer * n_chan:(layer + 1) * n_chan] = gate[begin:begin + rows]
        for col in range(0, n_chan, COLS):
            res = jnp.dot(gate[:m], wres[layer, :, col:col + COLS], preferred_element_type=F32).reshape(n_seq, size, COLS)
            near[:, lo:hi, col:col + COLS] = near[:, lo:hi, col:col + COLS] + res
        if layer < n_near - 1:
            @pl.when(me == 0)
            def _():
                near[:, :EDGE] = zero_edge

            @pl.when(me == last)
            def _():
                near[:, EDGE + rows:] = zero_edge

    for seq in range(n_seq):
        own = near[seq, EDGE:EDGE + rows].reshape(TILE, n_res, n_chan)
        out_blocks[seq * n_res:(seq + 1) * n_res] = jnp.swapaxes(own, 0, 1)

    def mid_copy(dst, src):
        return pltpu.make_async_remote_copy(src_ref=out_blocks.at[dst], dst_ref=far.at[pl.ds(pl.multiple_of(pad + src * TILE, TILE), TILE)],
                                            send_sem=mid_send.at[dst], recv_sem=mid_recv.at[src], device_id={'sp': dst}, device_id_type=MESH)

    @pl.loop(1, n_dev)
    def _(k):
        mid_copy(lax.rem(me + k, n_dev), me).start()

    far[pl.ds(pl.multiple_of(pad + me * TILE, TILE), TILE)] = out_blocks[me]

    for col in range(0, n_skip, COLS):
        skip = jnp.zeros((n_seq * rows, COLS), F32)
        for layer in range(n_near):
            skip = skip + jnp.dot(near_gate[:, layer * n_chan:(layer + 1) * n_chan], wskip[layer, :, col:col + COLS], preferred_element_type=F32)
        near_skip[:, :, col:col + COLS] = skip.reshape(n_seq, rows, COLS)
    skip_copy = pltpu.make_async_copy(near_skip, skip_out, own_sem.at[2])
    skip_copy.start()

    @pl.loop(1, n_dev)
    def _(k):
        src = lax.rem(me + n_dev - k, n_dev)
        mid_copy(lax.rem(me + k, n_dev), src).wait_recv()

    def end_copy(which, dst, src):
        source = far.at[pl.ds(pl.multiple_of(pad + dst * TILE, TILE), TILE)] if which == 0 else far_skip.at[pl.ds(pl.multiple_of(dst * TILE, TILE), TILE)]
        return pltpu.make_async_remote_copy(src_ref=source, dst_ref=(home_h, home_s)[which].at[src],
                                            send_sem=end_send.at[which, dst], recv_sem=end_recv.at[which, src], device_id={'sp': dst}, device_id_type=MESH)

    def own_copy(which):
        source = far.at[pl.ds(pl.multiple_of(pad + me * TILE, TILE), TILE)] if which == 0 else far_skip.at[pl.ds(pl.multiple_of(me * TILE, TILE), TILE)]
        return pltpu.make_async_copy(source, (home_h, home_s)[which].at[me], own_sem.at[which])

    def send_home(which):
        @pl.loop(1, n_dev)
        def _(k):
            end_copy(which, lax.rem(me + k, n_dev), me).start()

        own_copy(which).start()

    for layer in range(n_near, n_layers):
        dist = 2 ** layer // n_res
        for tap in range(3):
            off = pad + (tap - 1) * dist
            lhs[:far_rows, tap * n_chan:(tap + 1) * n_chan] = far[off:off + far_rows].astype(BF16)
        for copy in weight_copies(layer):
            copy.wait()
        gated_layer(layer, far_rows)
        for col in range(0, n_chan, COLS):
            res = jnp.dot(gate[:far_rows], wres[layer, :, col:col + COLS], preferred_element_type=F32)
            far[pad:pad + far_rows, col:col + COLS] = far[pad:pad + far_rows, col:col + COLS] + res
        if layer == n_layers - 1:
            send_home(0)
        for col in range(0, n_skip, COLS):
            skip = jnp.dot(gate[:far_rows], wskip[layer, :, col:col + COLS], preferred_element_type=F32)
            if layer > n_near:
                skip = far_skip[:, col:col + COLS] + skip
            far_skip[:, col:col + COLS] = skip

    send_home(1)

    for which in range(2):
        @pl.loop(1, n_dev)
        def _(k):
            end_copy(which, lax.rem(me + k, n_dev), lax.rem(me + n_dev - k, n_dev)).wait_recv()

    skip_copy.wait()
    own_copy(0).wait()
    own_copy(1).wait()

    @pl.when(me < last)
    def _():
        to_next().wait_send()

    @pl.when(me > 0)
    def _():
        to_prev().wait_send()

    @pl.loop(1, n_dev)
    def _(k):
        dst = lax.rem(me + k, n_dev)
        mid_copy(dst, me).wait_send()
        end_copy(0, dst, me).wait_send()
        end_copy(1, dst, me).wait_send()


def assemble_kernel(h_blocks, s_blocks, skip, h_out, s_out):
    n_res = h_blocks.shape[0]
    h_out[0] = jnp.swapaxes(h_blocks[...], 0, 1).reshape(h_out.shape[1:])
    s_out[0] = jnp.swapaxes(s_blocks[...], 0, 1).reshape(s_out.shape[1:]) + skip[0]


def solution(mesh):
    n_dev = mesh.shape['sp']
    act_spec = P('dp', 'sp', None)

    def local_stack(x, w_in, w_res, w_skip):
        n_seq, rows, n_chan = x.shape
        n_layers, n_skip = w_in.shape[0], w_skip.shape[2]
        n_res = n_dev // n_seq
        n_near = n_res.bit_length() - 1
        far_rows = n_dev * rows // n_res
        pad = 2 ** (n_layers - 1) // n_res
        any_spec = pl.BlockSpec(memory_space=pl.ANY)
        m_max = n_seq * (rows + 2 * HALO)
        dma = pltpu.SemaphoreType.DMA
        home_h, home_s, skip = pl.pallas_call(
            functools.partial(stack_kernel, n_dev, n_near),
            out_shape=(jax.ShapeDtypeStruct((n_dev, TILE, n_chan), F32), jax.ShapeDtypeStruct((n_dev, TILE, n_skip), F32),
                       jax.ShapeDtypeStruct((n_seq, rows, n_skip), F32)),
            in_specs=[any_spec] * 4,
            out_specs=[any_spec] * 3,
            scratch_shapes=[
                pltpu.VMEM(w_in.shape, BF16), pltpu.VMEM(w_res.shape, BF16), pltpu.VMEM(w_skip.shape, BF16),
                pltpu.VMEM(x.shape, BF16), pltpu.VMEM((n_seq, HALO, n_chan), BF16), pltpu.VMEM((n_seq, HALO, n_chan), BF16),
                pltpu.VMEM((n_seq, rows + 2 * EDGE, n_chan), F32), pltpu.VMEM((n_seq, rows, n_skip), F32),
                pltpu.VMEM((n_dev, TILE, n_chan), F32),
                pltpu.VMEM((far_rows + 2 * pad, n_chan), F32), pltpu.VMEM((far_rows, n_skip), F32),
                pltpu.VMEM((m_max, 3 * n_chan), BF16), pltpu.VMEM((m_max, n_chan), BF16), pltpu.VMEM((n_seq * rows, n_near * n_chan), BF16),
                dma, dma((3,)), dma((n_layers, 3)), dma((2,)), dma((2,)), dma((n_dev,)), dma((n_dev,)), dma((2, n_dev)), dma((2, n_dev)),
            ],
            compiler_params=pltpu.CompilerParams(collective_id=0, has_side_effects=True, vmem_limit_bytes=63 * 2 ** 20),
            name='dilated_stack',
        )(x, w_in, w_res, w_skip)
        blocks = lambda width: pl.BlockSpec((n_res, TILE, width), lambda i: (i, 0, 0))
        whole = lambda width: pl.BlockSpec((1, rows, width), lambda i: (i, 0, 0))
        return pl.pallas_call(
            assemble_kernel,
            grid=(n_seq,),
            out_shape=(jax.ShapeDtypeStruct((n_seq, rows, n_chan), F32), jax.ShapeDtypeStruct((n_seq, rows, n_skip), F32)),
            in_specs=[blocks(n_chan), blocks(n_skip), whole(n_skip)],
            out_specs=(whole(n_chan), whole(n_skip)),
            name='assemble',
        )(home_h, home_s, skip)

    return jax.shard_map(local_stack, mesh=mesh, in_specs=(act_spec, P(), P(), P()), out_specs=(act_spec, act_spec), check_vma=False)
```

```python
import functools

import jax
import jax.numpy as jnp
from jax import lax
from jax.experimental import pallas as pl
from jax.experimental.pallas import tpu as pltpu
from jax.sharding import PartitionSpec as P

MESH = pl.DeviceIdType.MESH
F32, BF16 = jnp.float32, jnp.bfloat16
TILE = 8
ROW = 8
HALO = 8
EDGE = 16
COLS = 256


def stack_kernel(n_dev, n_near, xv, win_hbm, wres_hbm, wskip_hbm, home_h, home_s, skip_out, win, wres, wskip, halo_l, halo_r,
                 near, near_skip, out_blocks, far, far_skip, lhs, gate, near_gate,
                 own_sem, w_sem, halo_send, halo_recv, ready_sem, mid_send, mid_recv, end_send, end_recv):
    me = lax.axis_index('sp')
    n_seq, rows, n_chan = xv.shape
    n_skip = far_skip.shape[1]
    n_layers = win.shape[0]
    far_rows = far_skip.shape[0]
    pad = (far.shape[0] - far_rows) // 2
    n_res = rows // TILE
    last = n_dev - 1

    n_rows = n_dev // ROW
    row, col = me // ROW, lax.rem(me, ROW)
    barrier = pltpu.get_barrier_semaphore()

    def tell(sem, dst):
        pl.semaphore_signal(sem, inc=1, device_id={'sp': dst}, device_id_type=MESH)

    for k in range(1, ROW):
        tell(barrier, row * ROW + lax.rem(col + k, ROW))

    def column(k):
        return lax.rem(row + k, n_rows) * ROW + col

    for k in range(1, n_rows):
        tell(barrier, column(k))
    before = jnp.logical_and(col == 0, row > 0)
    after = jnp.logical_and(col == ROW - 1, row < n_rows - 1)

    @pl.when(before)
    def _():
        tell(barrier, me - 1)

    @pl.when(after)
    def _():
        tell(barrier, me + 1)

    def weight_copies(layer):
        return [pltpu.make_async_copy(win_hbm.at[layer], win.at[layer], w_sem.at[layer, 0]),
                pltpu.make_async_copy(wres_hbm.at[layer], wres.at[layer], w_sem.at[layer, 1]),
                pltpu.make_async_copy(wskip_hbm.at[layer], wskip.at[layer], w_sem.at[layer, 2])]

    zero_edge = jnp.zeros((n_seq, EDGE, n_chan), F32)
    near[:, :EDGE] = zero_edge
    near[:, EDGE + rows:] = zero_edge
    far[:pad] = jnp.zeros((pad, n_chan), F32)
    far[pad + far_rows:] = jnp.zeros((pad, n_chan), F32)

    for layer in range(n_near):
        for copy in weight_copies(layer):
            copy.start()
    pl.semaphore_wait(barrier, ROW + n_rows - 2 + jnp.where(before, 1, 0) + jnp.where(after, 1, 0))


    def to_next():
        return pltpu.make_async_remote_copy(src_ref=xv.at[:, pl.ds(rows - HALO, HALO)], dst_ref=halo_l, send_sem=halo_send.at[0],
                                            recv_sem=halo_recv.at[0], device_id={'sp': me + 1}, device_id_type=MESH)

    def to_prev():
        return pltpu.make_async_remote_copy(src_ref=xv.at[:, pl.ds(0, HALO)], dst_ref=halo_r, send_sem=halo_send.at[1],
                                            recv_sem=halo_recv.at[1], device_id={'sp': me - 1}, device_id_type=MESH)

    @pl.when(me < last)
    def _():
        to_next().start()

    @pl.when(me > 0)
    def _():
        to_prev().start()

    for k in range(1, n_rows):
        tell(ready_sem, column(k))
    near[:, EDGE:EDGE + rows] = xv[...].astype(F32)

    @pl.when(me > 0)
    def _():
        to_next().wait_recv()
        near[:, EDGE - HALO:EDGE] = halo_l[...].astype(F32)

    @pl.when(me < last)
    def _():
        to_prev().wait_recv()
        near[:, EDGE + rows:EDGE + rows + HALO] = halo_r[...].astype(F32)

    def gated_layer(layer, m):
        w = win.at[layer]
        for col in range(0, n_chan, COLS):
            f = jnp.zeros((m, COLS), F32)
            g = jnp.zeros((m, COLS), F32)
            for tap in range(3):
                op = lhs[:m, tap * n_chan:(tap + 1) * n_chan]
                f = f + jnp.dot(op, w[tap, :, col:col + COLS], preferred_element_type=F32)
                g = g + jnp.dot(op, w[tap, :, n_chan + col:n_chan + col + COLS], preferred_element_type=F32)
            gate[:m, col:col + COLS] = (jnp.tanh(f) * (0.5 * jnp.tanh(0.5 * g) + 0.5)).astype(BF16)

    for layer in range(n_near):
        dist = 2 ** layer
        lo, hi = (EDGE - HALO, EDGE + rows + HALO) if layer < n_near - 1 else (EDGE, EDGE + rows)
        size = hi - lo
        m = n_seq * size
        for tap in range(3):
            off = lo + (tap - 1) * dist
            for seq in range(n_seq):
                lhs[seq * size:(seq + 1) * size, tap * n_chan:(tap + 1) * n_chan] = near[seq, off:off + size].astype(BF16)
        for copy in weight_copies(layer):
            copy.wait()
        if layer == n_near - 1:
            for later in range(n_near, n_layers):
                for copy in weight_copies(later):
                    copy.start()
        gated_layer(layer, m)
        for seq in range(n_seq):
            begin = seq * size + EDGE - lo
            near_gate[seq * rows:(seq + 1) * rows, layer * n_chan:(layer + 1) * n_chan] = gate[begin:begin + rows]
        for col in range(0, n_chan, COLS):
            res = jnp.dot(gate[:m], wres[layer, :, col:col + COLS], preferred_element_type=F32).reshape(n_seq, size, COLS)
            near[:, lo:hi, col:col + COLS] = near[:, lo:hi, col:col + COLS] + res
        if layer < n_near - 1:
            @pl.when(me == 0)
            def _():
                near[:, :EDGE] = zero_edge

            @pl.when(me == last)
            def _():
                near[:, EDGE + rows:] = zero_edge

    for seq in range(n_seq):
        own = near[seq, EDGE:EDGE + rows].reshape(TILE, n_res, n_chan)
        out_blocks[seq * n_res:(seq + 1) * n_res] = jnp.swapaxes(own, 0, 1)

    def mid_copy(dst, src):
        return pltpu.make_async_remote_copy(src_ref=out_blocks.at[dst], dst_ref=far.at[pl.ds(pl.multiple_of(pad + src * TILE, TILE), TILE)],
                                            send_sem=mid_send, recv_sem=mid_recv, device_id={'sp': dst}, device_id_type=MESH)

    pl.semaphore_wait(ready_sem, n_rows - 1)

    @pl.loop(1, n_dev)
    def _(k):
        mid_copy(lax.rem(me + k, n_dev), me).start()

    far[pl.ds(pl.multiple_of(pad + me * TILE, TILE), TILE)] = out_blocks[me]

    for col in range(0, n_skip, COLS):
        skip = jnp.zeros((n_seq * rows, COLS), F32)
        for layer in range(n_near):
            skip = skip + jnp.dot(near_gate[:, layer * n_chan:(layer + 1) * n_chan], wskip[layer, :, col:col + COLS], preferred_element_type=F32)
        near_skip[:, :, col:col + COLS] = skip.reshape(n_seq, rows, COLS)
    skip_copy = pltpu.make_async_copy(near_skip, skip_out, own_sem.at[2])
    skip_copy.start()

    others = pl.ds(0, n_dev - 1)
    pltpu.make_async_copy(out_blocks.at[others], out_blocks.at[others], mid_recv).wait()

    def end_copy(which, dst, src):
        source = far.at[pl.ds(pl.multiple_of(pad + dst * TILE, TILE), TILE)] if which == 0 else far_skip.at[pl.ds(pl.multiple_of(dst * TILE, TILE), TILE)]
        return pltpu.make_async_remote_copy(src_ref=source, dst_ref=(home_h, home_s)[which].at[src],
                                            send_sem=end_send.at[which], recv_sem=end_recv.at[which], device_id={'sp': dst}, device_id_type=MESH)

    def own_copy(which):
        source = far.at[pl.ds(pl.multiple_of(pad + me * TILE, TILE), TILE)] if which == 0 else far_skip.at[pl.ds(pl.multiple_of(me * TILE, TILE), TILE)]
        return pltpu.make_async_copy(source, (home_h, home_s)[which].at[me], own_sem.at[which])

    def send_home(which):
        @pl.loop(1, n_dev)
        def _(k):
            end_copy(which, lax.rem(me + k, n_dev), me).start()

        own_copy(which).start()

    for layer in range(n_near, n_layers):
        dist = 2 ** layer // n_res
        for tap in range(3):
            off = pad + (tap - 1) * dist
            lhs[:far_rows, tap * n_chan:(tap + 1) * n_chan] = far[off:off + far_rows].astype(BF16)
        for copy in weight_copies(layer):
            copy.wait()
        gated_layer(layer, far_rows)
        for col in range(0, n_chan, COLS):
            res = jnp.dot(gate[:far_rows], wres[layer, :, col:col + COLS], preferred_element_type=F32)
            far[pad:pad + far_rows, col:col + COLS] = far[pad:pad + far_rows, col:col + COLS] + res
        if layer == n_layers - 1:
            send_home(0)
        for col in range(0, n_skip, COLS):
            skip = jnp.dot(gate[:far_rows], wskip[layer, :, col:col + COLS], preferred_element_type=F32)
            if layer > n_near:
                skip = far_skip[:, col:col + COLS] + skip
            far_skip[:, col:col + COLS] = skip

    send_home(1)

    pltpu.make_async_copy(out_blocks.at[others], out_blocks.at[others], mid_send).wait()
    for which in range(2):
        blocks = (home_h, home_s)[which].at[others]
        pltpu.make_async_copy(blocks, blocks, end_recv.at[which]).wait()
    for which in range(2):
        blocks = (home_h, home_s)[which].at[others]
        pltpu.make_async_copy(blocks, blocks, end_send.at[which]).wait()
    skip_copy.wait()
    own_copy(0).wait()
    own_copy(1).wait()

    @pl.when(me < last)
    def _():
        to_next().wait_send()

    @pl.when(me > 0)
    def _():
        to_prev().wait_send()


def assemble_kernel(h_blocks, s_blocks, skip, h_out, s_out, h_rows, s_rows, sems):
    n_seq, rows, n_chan = h_rows.shape
    n_res = h_blocks.shape[0] // n_seq

    def copies(seq):
        return (pltpu.make_async_copy(h_rows.at[seq], h_out.at[seq], sems.at[0, seq]),
                pltpu.make_async_copy(s_rows.at[seq], s_out.at[seq], sems.at[1, seq]))

    for seq in range(n_seq):
        blocks = slice(seq * n_res, (seq + 1) * n_res)
        h_rows[seq] = jnp.swapaxes(h_blocks[blocks], 0, 1).reshape(rows, n_chan)
        copies(seq)[0].start()
        s_rows[seq] = jnp.swapaxes(s_blocks[blocks], 0, 1).reshape(rows, s_rows.shape[2]) + skip[seq]
        copies(seq)[1].start()
    for seq in range(n_seq):
        for copy in copies(seq):
            copy.wait()


def solution(mesh):
    n_dev = mesh.shape['sp']
    act_spec = P('dp', 'sp', None)

    def local_stack(x, w_in, w_res, w_skip):
        n_seq, rows, n_chan = x.shape
        n_layers, n_skip = w_in.shape[0], w_skip.shape[2]
        n_res = n_dev // n_seq
        n_near = n_res.bit_length() - 1
        far_rows = n_dev * rows // n_res
        pad = 2 ** (n_layers - 1) // n_res
        any_spec = pl.BlockSpec(memory_space=pl.ANY)
        m_max = n_seq * (rows + 2 * HALO)
        dma = pltpu.SemaphoreType.DMA
        home_h, home_s, skip = pl.pallas_call(
            functools.partial(stack_kernel, n_dev, n_near),
            out_shape=(jax.ShapeDtypeStruct((n_dev, TILE, n_chan), F32), jax.ShapeDtypeStruct((n_dev, TILE, n_skip), F32),
                       jax.ShapeDtypeStruct((n_seq, rows, n_skip), F32)),
            in_specs=[pl.BlockSpec(memory_space=pltpu.VMEM)] + [any_spec] * 3,
            out_specs=[any_spec] * 3,
            scratch_shapes=[
                pltpu.VMEM(w_in.shape, BF16), pltpu.VMEM(w_res.shape, BF16), pltpu.VMEM(w_skip.shape, BF16),
                pltpu.VMEM((n_seq, HALO, n_chan), BF16), pltpu.VMEM((n_seq, HALO, n_chan), BF16),
                pltpu.VMEM((n_seq, rows + 2 * EDGE, n_chan), F32), pltpu.VMEM((n_seq, rows, n_skip), F32),
                pltpu.VMEM((n_dev, TILE, n_chan), F32),
                pltpu.VMEM((far_rows + 2 * pad, n_chan), F32), pltpu.VMEM((far_rows, n_skip), F32),
                pltpu.VMEM((m_max, 3 * n_chan), BF16), pltpu.VMEM((m_max, n_chan), BF16), pltpu.VMEM((n_seq * rows, n_near * n_chan), BF16),
                dma((3,)), dma((n_layers, 3)), dma((2,)), dma((2,)), pltpu.SemaphoreType.REGULAR, dma, dma, dma((2,)), dma((2,)),
            ],
            compiler_params=pltpu.CompilerParams(collective_id=0, has_side_effects=True, vmem_limit_bytes=52 * 2 ** 20),
            name='dilated_stack',
        )(x, w_in, w_res, w_skip)
        return pl.pallas_call(
            assemble_kernel,
            out_shape=(jax.ShapeDtypeStruct((n_seq, rows, n_chan), F32), jax.ShapeDtypeStruct((n_seq, rows, n_skip), F32)),
            in_specs=[pl.BlockSpec(memory_space=pltpu.VMEM)] * 3,
            out_specs=[any_spec] * 2,
            scratch_shapes=[pltpu.VMEM((n_seq, rows, n_chan), F32), pltpu.VMEM((n_seq, rows, n_skip), F32), dma((2, n_seq))],
            compiler_params=pltpu.CompilerParams(vmem_limit_bytes=4 * 2 ** 20),
            name='assemble',
        )(home_h, home_s, skip)

    return jax.shard_map(local_stack, mesh=mesh, in_specs=(act_spec, P(), P(), P()), out_specs=(act_spec, act_spec), check_vma=False)
```

```python
import functools

import jax
import jax.numpy as jnp
from jax import lax
from jax.experimental import pallas as pl
from jax.experimental.pallas import tpu as pltpu
from jax.sharding import PartitionSpec as P

MESH = pl.DeviceIdType.MESH
F32, BF16 = jnp.float32, jnp.bfloat16
TILE = 8
AHEAD = 3
ROW = 8
HALO = 8
EDGE = 16
COLS = 256


def stack_kernel(n_dev, n_near, xv, win_hbm, wres_hbm, wskip_hbm, home_h, home_s, skip_out, win, wres, wskip, halo_l, halo_r,
                 near, near_skip, out_blocks, far, far_skip, lhs, gate, near_gate,
                 own_sem, w_sem, halo_send, halo_recv, ready_sem, mid_send, mid_recv, end_send, end_recv):
    me = lax.axis_index('sp')
    n_seq, rows, n_chan = xv.shape
    n_skip = far_skip.shape[1]
    n_layers = win.shape[0]
    far_rows = far_skip.shape[0]
    pad = (far.shape[0] - far_rows) // 2
    n_res = rows // TILE
    last = n_dev - 1

    def weight_copies(layer):
        return [pltpu.make_async_copy(win_hbm.at[layer], win.at[layer], w_sem.at[layer, 0]),
                pltpu.make_async_copy(wres_hbm.at[layer], wres.at[layer], w_sem.at[layer, 1]),
                pltpu.make_async_copy(wskip_hbm.at[layer], wskip.at[layer], w_sem.at[layer, 2])]

    def start_weights(*layers):
        for layer in layers:
            for copy in weight_copies(layer):
                copy.start()

    start_weights(0)

    n_rows = n_dev // ROW
    row, col = me // ROW, lax.rem(me, ROW)
    barrier = pltpu.get_barrier_semaphore()

    def tell(sem, dst):
        pl.semaphore_signal(sem, inc=1, device_id={'sp': dst}, device_id_type=MESH)

    for k in range(1, ROW):
        tell(barrier, row * ROW + lax.rem(col + k, ROW))

    up, down = row > 0, row < n_rows - 1

    def tell_column(sem):
        @pl.when(up)
        def _():
            tell(sem, me - ROW)

        @pl.when(down)
        def _():
            tell(sem, me + ROW)

    tell_column(barrier)
    before, after = jnp.logical_and(col == 0, up), jnp.logical_and(col == ROW - 1, down)

    @pl.when(before)
    def _():
        tell(barrier, me - 1)

    @pl.when(after)
    def _():
        tell(barrier, me + 1)

    def count(*conditions):
        return sum(jnp.where(c, 1, 0) for c in conditions)

    def heard_column(step):
        pl.semaphore_wait(ready_sem.at[step - 1], count(up, down))
        if step < n_rows - 1:
            tell_column(ready_sem.at[step])

    zero_edge = jnp.zeros((n_seq, EDGE, n_chan), F32)
    near[:, :EDGE] = zero_edge
    near[:, EDGE + rows:] = zero_edge
    far[:pad] = jnp.zeros((pad, n_chan), F32)
    far[pad + far_rows:] = jnp.zeros((pad, n_chan), F32)

    pl.semaphore_wait(barrier, ROW - 1 + count(up, down, before, after))
    tell_column(ready_sem.at[0])
    start_weights(*range(1, n_near))


    def to_next():
        return pltpu.make_async_remote_copy(src_ref=xv.at[:, pl.ds(rows - HALO, HALO)], dst_ref=halo_l, send_sem=halo_send.at[0],
                                            recv_sem=halo_recv.at[0], device_id={'sp': me + 1}, device_id_type=MESH)

    def to_prev():
        return pltpu.make_async_remote_copy(src_ref=xv.at[:, pl.ds(0, HALO)], dst_ref=halo_r, send_sem=halo_send.at[1],
                                            recv_sem=halo_recv.at[1], device_id={'sp': me - 1}, device_id_type=MESH)

    @pl.when(me < last)
    def _():
        to_next().start()

    @pl.when(me > 0)
    def _():
        to_prev().start()

    near[:, EDGE:EDGE + rows] = xv[...].astype(F32)

    @pl.when(me > 0)
    def _():
        to_next().wait_recv()
        near[:, EDGE - HALO:EDGE] = halo_l[...].astype(F32)

    @pl.when(me < last)
    def _():
        to_prev().wait_recv()
        near[:, EDGE + rows:EDGE + rows + HALO] = halo_r[...].astype(F32)

    def gated_layer(layer, m):
        w = win.at[layer]
        for col in range(0, n_chan, COLS):
            f = jnp.zeros((m, COLS), F32)
            g = jnp.zeros((m, COLS), F32)
            for tap in range(3):
                op = lhs[:m, tap * n_chan:(tap + 1) * n_chan]
                f = f + jnp.dot(op, w[tap, :, col:col + COLS], preferred_element_type=F32)
                g = g + jnp.dot(op, w[tap, :, n_chan + col:n_chan + col + COLS], preferred_element_type=F32)
            gate[:m, col:col + COLS] = (jnp.tanh(f) * (0.5 * jnp.tanh(0.5 * g) + 0.5)).astype(BF16)

    for layer in range(n_near):
        dist = 2 ** layer
        lo, hi = (EDGE - HALO, EDGE + rows + HALO) if layer < n_near - 1 else (EDGE, EDGE + rows)
        size = hi - lo
        m = n_seq * size
        for tap in range(3):
            off = lo + (tap - 1) * dist
            for seq in range(n_seq):
                lhs[seq * size:(seq + 1) * size, tap * n_chan:(tap + 1) * n_chan] = near[seq, off:off + size].astype(BF16)
        for copy in weight_copies(layer):
            copy.wait()
        if layer == n_near - 2:
            start_weights(*range(n_near, n_near + AHEAD))
        if layer == n_near - 1:
            start_weights(*range(n_near + AHEAD, n_layers))
        gated_layer(layer, m)
        for seq in range(n_seq):
            begin = seq * size + EDGE - lo
            near_gate[seq * rows:(seq + 1) * rows, layer * n_chan:(layer + 1) * n_chan] = gate[begin:begin + rows]
        for col in range(0, n_chan, COLS):
            res = jnp.dot(gate[:m], wres[layer, :, col:col + COLS], preferred_element_type=F32).reshape(n_seq, size, COLS)
            near[:, lo:hi, col:col + COLS] = near[:, lo:hi, col:col + COLS] + res
        if layer < n_near - 1:
            if layer + 1 < n_rows:
                heard_column(layer + 1)

            @pl.when(me == 0)
            def _():
                near[:, :EDGE] = zero_edge

            @pl.when(me == last)
            def _():
                near[:, EDGE + rows:] = zero_edge

    for seq in range(n_seq):
        own = near[seq, EDGE:EDGE + rows].reshape(TILE, n_res, n_chan)
        out_blocks[seq * n_res:(seq + 1) * n_res] = jnp.swapaxes(own, 0, 1)

    def mid_copy(dst, src):
        return pltpu.make_async_remote_copy(src_ref=out_blocks.at[dst], dst_ref=far.at[pl.ds(pl.multiple_of(pad + src * TILE, TILE), TILE)],
                                            send_sem=mid_send, recv_sem=mid_recv, device_id={'sp': dst}, device_id_type=MESH)

    for step in range(n_near, n_rows):
        heard_column(step)

    @pl.loop(1, n_dev)
    def _(k):
        mid_copy(lax.rem(me + k, n_dev), me).start()

    far[pl.ds(pl.multiple_of(pad + me * TILE, TILE), TILE)] = out_blocks[me]

    for col in range(0, n_skip, COLS):
        skip = jnp.zeros((n_seq * rows, COLS), F32)
        for layer in range(n_near):
            skip = skip + jnp.dot(near_gate[:, layer * n_chan:(layer + 1) * n_chan], wskip[layer, :, col:col + COLS], preferred_element_type=F32)
        near_skip[:, :, col:col + COLS] = skip.reshape(n_seq, rows, COLS)
    skip_copy = pltpu.make_async_copy(near_skip, skip_out, own_sem.at[2])
    skip_copy.start()

    for layer in range(n_near, n_layers):
        for copy in weight_copies(layer):
            copy.wait()
    others = pl.ds(0, n_dev - 1)
    pltpu.make_async_copy(out_blocks.at[others], out_blocks.at[others], mid_recv).wait()

    def end_copy(which, dst, src):
        source = far.at[pl.ds(pl.multiple_of(pad + dst * TILE, TILE), TILE)] if which == 0 else far_skip.at[pl.ds(pl.multiple_of(dst * TILE, TILE), TILE)]
        return pltpu.make_async_remote_copy(src_ref=source, dst_ref=(home_h, home_s)[which].at[src],
                                            send_sem=end_send.at[which], recv_sem=end_recv.at[which], device_id={'sp': dst}, device_id_type=MESH)

    def own_copy(which):
        source = far.at[pl.ds(pl.multiple_of(pad + me * TILE, TILE), TILE)] if which == 0 else far_skip.at[pl.ds(pl.multiple_of(me * TILE, TILE), TILE)]
        return pltpu.make_async_copy(source, (home_h, home_s)[which].at[me], own_sem.at[which])

    def send_home(which):
        @pl.loop(0, n_dev)
        def _(k):
            dst = k + 1 - 2 * lax.rem(k, 2)

            @pl.when(dst != me)
            def _():
                end_copy(which, dst, me).start()

        own_copy(which).start()

    for layer in range(n_near, n_layers):
        dist = 2 ** layer // n_res
        for tap in range(3):
            off = pad + (tap - 1) * dist
            lhs[:far_rows, tap * n_chan:(tap + 1) * n_chan] = far[off:off + far_rows].astype(BF16)
        gated_layer(layer, far_rows)
        for col in range(0, n_chan, COLS):
            res = jnp.dot(gate[:far_rows], wres[layer, :, col:col + COLS], preferred_element_type=F32)
            far[pad:pad + far_rows, col:col + COLS] = far[pad:pad + far_rows, col:col + COLS] + res
        if layer == n_layers - 1:
            send_home(0)
        for col in range(0, n_skip, COLS):
            skip = jnp.dot(gate[:far_rows], wskip[layer, :, col:col + COLS], preferred_element_type=F32)
            if layer > n_near:
                skip = far_skip[:, col:col + COLS] + skip
            far_skip[:, col:col + COLS] = skip

    send_home(1)

    pltpu.make_async_copy(out_blocks.at[others], out_blocks.at[others], mid_send).wait()
    for which in range(2):
        blocks = (home_h, home_s)[which].at[others]
        pltpu.make_async_copy(blocks, blocks, end_recv.at[which]).wait()
    for which in range(2):
        blocks = (home_h, home_s)[which].at[others]
        pltpu.make_async_copy(blocks, blocks, end_send.at[which]).wait()
    skip_copy.wait()
    own_copy(0).wait()
    own_copy(1).wait()

    @pl.when(me < last)
    def _():
        to_next().wait_send()

    @pl.when(me > 0)
    def _():
        to_prev().wait_send()


def assemble_kernel(h_blocks, s_blocks, skip, h_out, s_out, h_rows, s_rows, sems):
    n_seq, rows, n_chan = h_rows.shape
    n_res = h_blocks.shape[0] // n_seq

    def copies(seq):
        return (pltpu.make_async_copy(h_rows.at[seq], h_out.at[seq], sems.at[0, seq]),
                pltpu.make_async_copy(s_rows.at[seq], s_out.at[seq], sems.at[1, seq]))

    for seq in range(n_seq):
        blocks = slice(seq * n_res, (seq + 1) * n_res)
        h_rows[seq] = jnp.swapaxes(h_blocks[blocks], 0, 1).reshape(rows, n_chan)
        copies(seq)[0].start()
        s_rows[seq] = jnp.swapaxes(s_blocks[blocks], 0, 1).reshape(rows, s_rows.shape[2]) + skip[seq]
        copies(seq)[1].start()
    for seq in range(n_seq):
        for copy in copies(seq):
            copy.wait()


def solution(mesh):
    n_dev = mesh.shape['sp']
    act_spec = P('dp', 'sp', None)

    def local_stack(x, w_in, w_res, w_skip):
        n_seq, rows, n_chan = x.shape
        n_layers, n_skip = w_in.shape[0], w_skip.shape[2]
        n_res = n_dev // n_seq
        n_near = n_res.bit_length() - 1
        far_rows = n_dev * rows // n_res
        pad = 2 ** (n_layers - 1) // n_res
        any_spec = pl.BlockSpec(memory_space=pl.ANY)
        m_max = n_seq * (rows + 2 * HALO)
        dma = pltpu.SemaphoreType.DMA
        home_h, home_s, skip = pl.pallas_call(
            functools.partial(stack_kernel, n_dev, n_near),
            out_shape=(jax.ShapeDtypeStruct((n_dev, TILE, n_chan), F32), jax.ShapeDtypeStruct((n_dev, TILE, n_skip), F32),
                       jax.ShapeDtypeStruct((n_seq, rows, n_skip), F32)),
            in_specs=[pl.BlockSpec(memory_space=pltpu.VMEM)] + [any_spec] * 3,
            out_specs=[any_spec] * 3,
            scratch_shapes=[
                pltpu.VMEM(w_in.shape, BF16), pltpu.VMEM(w_res.shape, BF16), pltpu.VMEM(w_skip.shape, BF16),
                pltpu.VMEM((n_seq, HALO, n_chan), BF16), pltpu.VMEM((n_seq, HALO, n_chan), BF16),
                pltpu.VMEM((n_seq, rows + 2 * EDGE, n_chan), F32), pltpu.VMEM((n_seq, rows, n_skip), F32),
                pltpu.VMEM((n_dev, TILE, n_chan), F32),
                pltpu.VMEM((far_rows + 2 * pad, n_chan), F32), pltpu.VMEM((far_rows, n_skip), F32),
                pltpu.VMEM((m_max, 3 * n_chan), BF16), pltpu.VMEM((m_max, n_chan), BF16), pltpu.VMEM((n_seq * rows, n_near * n_chan), BF16),
                dma((3,)), dma((n_layers, 3)), dma((2,)), dma((2,)), pltpu.SemaphoreType.REGULAR((max(n_dev // ROW - 1, 1),)), dma, dma, dma((2,)), dma((2,)),
            ],
            compiler_params=pltpu.CompilerParams(collective_id=0, has_side_effects=True, vmem_limit_bytes=52 * 2 ** 20),
            name='dilated_stack',
        )(x, w_in, w_res, w_skip)
        return pl.pallas_call(
            assemble_kernel,
            out_shape=(jax.ShapeDtypeStruct((n_seq, rows, n_chan), F32), jax.ShapeDtypeStruct((n_seq, rows, n_skip), F32)),
            in_specs=[pl.BlockSpec(memory_space=pltpu.VMEM)] * 3,
            out_specs=[any_spec] * 2,
            scratch_shapes=[pltpu.VMEM((n_seq, rows, n_chan), F32), pltpu.VMEM((n_seq, rows, n_skip), F32), dma((2, n_seq))],
            compiler_params=pltpu.CompilerParams(vmem_limit_bytes=4 * 2 ** 20),
            name='assemble',
        )(home_h, home_s, skip)

    return jax.shard_map(local_stack, mesh=mesh, in_specs=(act_spec, P(), P(), P()), out_specs=(act_spec, act_spec), check_vma=False)
```

```python
import functools

import jax
import jax.numpy as jnp
from jax import lax
from jax.experimental import pallas as pl
from jax.experimental.pallas import tpu as pltpu
from jax.sharding import PartitionSpec as P

MESH = pl.DeviceIdType.MESH
F32, BF16 = jnp.float32, jnp.bfloat16
TILE = 8
AHEAD = 3
ROW = 8
HALO = 16
EDGE = 24
GROUPS = 2
COLS = 256


def swap_halves(first, second):
    half = first.shape[1] // 2
    upper = lax.broadcasted_iota(jnp.int32, first.shape, 1) < half
    return jnp.where(upper, first, pltpu.roll(second, half, 1)), jnp.where(upper, pltpu.roll(first, half, 1), second)


def stack_kernel(n_dev, n_near, xv, win_hbm, wres_hbm, wskip_hbm, home, skip_out, win, wres, wskip, halo_l, halo_r,
                 near, near_skip, mid_out, mid_in, far, far_skip, end_out, lhs, gate, near_gate,
                 own_sem, w_sem, halo_send, halo_recv, ready_sem, mid_send, mid_recv, end_send, end_recv):
    me = lax.axis_index('sp')
    n_seq, rows, n_chan = xv.shape
    n_skip = far_skip.shape[2]
    n_layers = win.shape[0]
    far_rows = far_skip.shape[1]
    pad = (far.shape[1] - far_rows) // 2
    in_group = n_seq // GROUPS
    n_res = n_dev // in_group
    part = rows // n_res
    lanes = n_chan * part // TILE
    n_side = TILE // part
    last = n_dev - 1

    def weight_copies(layer):
        return [pltpu.make_async_copy(win_hbm.at[layer], win.at[layer], w_sem.at[layer, 0]),
                pltpu.make_async_copy(wres_hbm.at[layer], wres.at[layer], w_sem.at[layer, 1]),
                pltpu.make_async_copy(wskip_hbm.at[layer], wskip.at[layer], w_sem.at[layer, 2])]

    def start_weights(*layers):
        for layer in layers:
            for copy in weight_copies(layer):
                copy.start()

    start_weights(0)

    n_rows = n_dev // ROW
    row, col = me // ROW, lax.rem(me, ROW)
    barrier = pltpu.get_barrier_semaphore()

    def tell(sem, dst):
        pl.semaphore_signal(sem, inc=1, device_id={'sp': dst}, device_id_type=MESH)

    for k in range(1, ROW):
        tell(barrier, row * ROW + lax.rem(col + k, ROW))

    up, down = row > 0, row < n_rows - 1

    def tell_column(sem):
        @pl.when(up)
        def _():
            tell(sem, me - ROW)

        @pl.when(down)
        def _():
            tell(sem, me + ROW)

    tell_column(barrier)
    before, after = jnp.logical_and(col == 0, up), jnp.logical_and(col == ROW - 1, down)

    @pl.when(before)
    def _():
        tell(barrier, me - 1)

    @pl.when(after)
    def _():
        tell(barrier, me + 1)

    def count(*conditions):
        return sum(jnp.where(c, 1, 0) for c in conditions)

    def heard_column(step):
        pl.semaphore_wait(ready_sem.at[step - 1], count(up, down))
        if step < n_rows - 1:
            tell_column(ready_sem.at[step])

    zero_edge = jnp.zeros((n_seq, EDGE, n_chan), F32)
    near[:, :EDGE] = zero_edge
    near[:, EDGE + rows:] = zero_edge
    for group in range(GROUPS):
        far[group, :pad] = jnp.zeros((pad, n_chan), F32)
        far[group, pad + far_rows:] = jnp.zeros((pad, n_chan), F32)

    pl.semaphore_wait(barrier, ROW - 1 + count(up, down, before, after))
    tell_column(ready_sem.at[0])
    start_weights(*range(1, n_near - 1))


    def to_next():
        return pltpu.make_async_remote_copy(src_ref=xv.at[:, pl.ds(rows - HALO, HALO)], dst_ref=halo_l, send_sem=halo_send.at[0],
                                            recv_sem=halo_recv.at[0], device_id={'sp': me + 1}, device_id_type=MESH)

    def to_prev():
        return pltpu.make_async_remote_copy(src_ref=xv.at[:, pl.ds(0, HALO)], dst_ref=halo_r, send_sem=halo_send.at[1],
                                            recv_sem=halo_recv.at[1], device_id={'sp': me - 1}, device_id_type=MESH)

    @pl.when(me < last)
    def _():
        to_next().start()

    @pl.when(me > 0)
    def _():
        to_prev().start()

    near[:, EDGE:EDGE + rows] = xv[...].astype(F32)

    @pl.when(me > 0)
    def _():
        to_next().wait_recv()
        near[:, EDGE - HALO:EDGE] = halo_l[...].astype(F32)

    @pl.when(me < last)
    def _():
        to_prev().wait_recv()
        near[:, EDGE + rows:EDGE + rows + HALO] = halo_r[...].astype(F32)

    def gated_layer(layer, m):
        w = win.at[layer]
        for col in range(0, n_chan, COLS):
            f = jnp.zeros((m, COLS), F32)
            g = jnp.zeros((m, COLS), F32)
            for tap in range(3):
                op = lhs[:m, tap * n_chan:(tap + 1) * n_chan]
                f = f + jnp.dot(op, w[tap, :, col:col + COLS], preferred_element_type=F32)
                g = g + jnp.dot(op, w[tap, :, n_chan + col:n_chan + col + COLS], preferred_element_type=F32)
            gate[:m, col:col + COLS] = (jnp.tanh(f) * (0.5 * jnp.tanh(0.5 * g) + 0.5)).astype(BF16)

    start_weights(n_near - 1)

    def near_phase(group):
        seqs = range(group * in_group, (group + 1) * in_group)
        every = slice(group * in_group, (group + 1) * in_group)
        for layer in range(n_near):
            dist = 2 ** layer
            reach = -(-(2 ** n_near - 2 * dist) // TILE) * TILE
            lo, hi = EDGE - reach, EDGE + rows + reach
            size = hi - lo
            m = in_group * size
            for tap in range(3):
                off = lo + (tap - 1) * dist
                for at, seq in enumerate(seqs):
                    lhs[at * size:(at + 1) * size, tap * n_chan:(tap + 1) * n_chan] = near[seq, off:off + size].astype(BF16)
            if group == 0:
                for copy in weight_copies(layer):
                    copy.wait()
                if layer == 1:
                    start_weights(*range(n_near, n_near + AHEAD))
                if layer == n_near - 1:
                    start_weights(*range(n_near + AHEAD, n_layers))
            gated_layer(layer, m)
            for at, seq in enumerate(seqs):
                begin = at * size + EDGE - lo
                near_gate[seq * rows:(seq + 1) * rows, layer * n_chan:(layer + 1) * n_chan] = gate[begin:begin + rows]
            for col in range(0, n_chan, COLS):
                res = jnp.dot(gate[:m], wres[layer, :, col:col + COLS], preferred_element_type=F32).reshape(in_group, size, COLS)
                near[every, lo:hi, col:col + COLS] = near[every, lo:hi, col:col + COLS] + res
            if group == 0 and layer + 1 < n_rows:
                heard_column(layer + 1)
            if layer < n_near - 1:
                @pl.when(me == 0)
                def _():
                    near[every, :EDGE] = zero_edge[:in_group]

                @pl.when(me == last)
                def _():
                    near[every, EDGE + rows:] = zero_edge[:in_group]

        for at, seq in enumerate(seqs):
            for low in range(0, n_res, TILE):
                sides = [near[seq, EDGE:EDGE + rows, side * lanes:(side + 1) * lanes].reshape(part, n_res, lanes)[:, low:low + TILE]
                         for side in range(n_side)]
                mid_out[group, at * n_res + low:at * n_res + low + TILE] = jnp.swapaxes(jnp.concatenate(sides, axis=0), 0, 1)

    def mid_copy(group, dst):
        return pltpu.make_async_remote_copy(src_ref=mid_out.at[group, dst], dst_ref=mid_in.at[group, me], send_sem=mid_send.at[group],
                                            recv_sem=mid_recv.at[group], device_id={'sp': dst}, device_id_type=MESH)

    def send_mid(group):
        @pl.loop(1, n_dev)
        def _(k):
            mid_copy(group, lax.rem(me + k, n_dev)).start()

        mid_in[group, me] = mid_out[group, me]

    for group in range(GROUPS):
        near_phase(group)
        if group == 0:
            for step in range(n_near + 1, n_rows):
                heard_column(step)
        send_mid(group)

    for col in range(0, n_skip, COLS):
        skip = jnp.zeros((n_seq * rows, COLS), F32)
        for layer in range(n_near):
            skip = skip + jnp.dot(near_gate[:, layer * n_chan:(layer + 1) * n_chan], wskip[layer, :, col:col + COLS], preferred_element_type=F32)
        near_skip[:, :, col:col + COLS] = skip.reshape(n_seq, rows, COLS)
    skip_copy = pltpu.make_async_copy(near_skip, skip_out, own_sem.at[GROUPS])
    skip_copy.start()

    def end_copy(group, dst):
        return pltpu.make_async_remote_copy(src_ref=end_out.at[group, dst // 2, lax.rem(dst, 2)], dst_ref=home.at[group, me],
                                            send_sem=end_send.at[group], recv_sem=end_recv.at[group], device_id={'sp': dst}, device_id_type=MESH)

    def own_copy(group):
        return pltpu.make_async_copy(end_out.at[group, me // 2, lax.rem(me, 2)], home.at[group, me], own_sem.at[group])

    def send_home(group):
        @pl.loop(0, n_dev)
        def _(k):
            dst = k + 1 - 2 * lax.rem(k, 2)

            @pl.when(dst != me)
            def _():
                end_copy(group, dst).start()

        own_copy(group).start()

    others = pl.ds(0, n_dev - 1)

    def wait_all(ref, sem):
        pltpu.make_async_copy(ref.at[others], ref.at[others], sem).wait()

    for group in range(GROUPS):
        wait_all(mid_in.at[group], mid_recv.at[group])
        blocks = mid_in[group].reshape(n_dev // 2, 2, TILE, lanes)
        for side, value in enumerate(swap_halves(blocks[:, 0], blocks[:, 1])):
            far[group, pad:pad + far_rows, side * lanes:(side + 1) * lanes] = value.reshape(far_rows, lanes)
        for layer in range(n_near, n_layers):
            dist = 2 ** layer // n_res
            for tap in range(3):
                off = pad + (tap - 1) * dist
                lhs[:far_rows, tap * n_chan:(tap + 1) * n_chan] = far[group, off:off + far_rows].astype(BF16)
            if group == 0:
                for copy in weight_copies(layer):
                    copy.wait()
            gated_layer(layer, far_rows)
            for col in range(0, n_chan, COLS):
                res = jnp.dot(gate[:far_rows], wres[layer, :, col:col + COLS], preferred_element_type=F32)
                far[group, pad:pad + far_rows, col:col + COLS] = far[group, pad:pad + far_rows, col:col + COLS] + res
            for col in range(0, n_skip, COLS):
                skip = jnp.dot(gate[:far_rows], wskip[layer, :, col:col + COLS], preferred_element_type=F32)
                if layer > n_near:
                    skip = far_skip[group, :, col:col + COLS] + skip
                far_skip[group, :, col:col + COLS] = skip
        for which, value in enumerate((far[group, pad:pad + far_rows], far_skip[group])):
            sides = [value[:, side * lanes:(side + 1) * lanes].reshape(n_dev // 2, TILE, lanes) for side in range(n_side)]
            for at, block in enumerate(swap_halves(*sides)):
                end_out[group, :, at, which * TILE:(which + 1) * TILE] = block
        send_home(group)

    for group in range(GROUPS):
        wait_all(mid_out.at[group], mid_send.at[group])
    for group in range(GROUPS):
        wait_all(home.at[group], end_recv.at[group])
    for group in range(GROUPS):
        wait_all(home.at[group], end_send.at[group])
        own_copy(group).wait()
    skip_copy.wait()

    @pl.when(me < last)
    def _():
        to_next().wait_send()

    @pl.when(me > 0)
    def _():
        to_prev().wait_send()


def assemble_kernel(home, skip, h_out, s_out, h_rows, s_rows, sems):
    n_seq, rows, n_chan = h_rows.shape
    lanes = home.shape[3]
    in_group = n_seq // GROUPS
    n_res = home.shape[1] // in_group
    part = rows // n_res

    def copies(seq):
        return (pltpu.make_async_copy(h_rows.at[seq], h_out.at[seq], sems.at[0, seq]),
                pltpu.make_async_copy(s_rows.at[seq], s_out.at[seq], sems.at[1, seq]))

    for seq in range(n_seq):
        group, at = seq // in_group, seq % in_group
        for which, out in enumerate((h_rows, s_rows)):
            for low in range(0, n_res, TILE):
                blocks = home[group, at * n_res + low:at * n_res + low + TILE, which * TILE:(which + 1) * TILE]
                turned = jnp.swapaxes(blocks, 0, 1)
                for k in range(TILE):
                    begin, side = k % part * n_res + low, k // part
                    value = turned[k]
                    if which == 1:
                        value = value + skip[seq, begin:begin + TILE, side * lanes:(side + 1) * lanes]
                    out[seq, begin:begin + TILE, side * lanes:(side + 1) * lanes] = value
            copies(seq)[which].start()
    for seq in range(n_seq):
        for copy in copies(seq):
            copy.wait()


def solution(mesh):
    n_dev = mesh.shape['sp']
    act_spec = P('dp', 'sp', None)

    def local_stack(x, w_in, w_res, w_skip):
        n_seq, rows, n_chan = x.shape
        n_layers, n_skip = w_in.shape[0], w_skip.shape[2]
        n_res = n_dev * GROUPS // n_seq
        n_near = n_res.bit_length() - 1
        far_rows = n_dev * rows // n_res
        pad = 2 ** (n_layers - 1) // n_res
        part = rows // n_res
        lanes = n_chan * part // TILE
        assert TILE == 2 * part and n_skip == n_chan
        any_spec = pl.BlockSpec(memory_space=pl.ANY)
        m_max = n_seq // GROUPS * (rows + 2 * HALO)
        dma = pltpu.SemaphoreType.DMA
        home, skip = pl.pallas_call(
            functools.partial(stack_kernel, n_dev, n_near),
            out_shape=(jax.ShapeDtypeStruct((GROUPS, n_dev, 2 * TILE, lanes), F32), jax.ShapeDtypeStruct((n_seq, rows, n_skip), F32)),
            in_specs=[pl.BlockSpec(memory_space=pltpu.VMEM)] + [any_spec] * 3,
            out_specs=[any_spec] * 2,
            scratch_shapes=[
                pltpu.VMEM(w_in.shape, BF16), pltpu.VMEM(w_res.shape, BF16), pltpu.VMEM(w_skip.shape, BF16),
                pltpu.VMEM((n_seq, HALO, n_chan), BF16), pltpu.VMEM((n_seq, HALO, n_chan), BF16),
                pltpu.VMEM((n_seq, rows + 2 * EDGE, n_chan), F32), pltpu.VMEM((n_seq, rows, n_skip), F32),
                pltpu.VMEM((GROUPS, n_dev, TILE, lanes), F32), pltpu.VMEM((GROUPS, n_dev, TILE, lanes), F32),
                pltpu.VMEM((GROUPS, far_rows + 2 * pad, n_chan), F32), pltpu.VMEM((GROUPS, far_rows, n_skip), F32),
                pltpu.VMEM((GROUPS, n_dev // 2, 2, 2 * TILE, lanes), F32),
                pltpu.VMEM((m_max, 3 * n_chan), BF16), pltpu.VMEM((m_max, n_chan), BF16), pltpu.VMEM((n_seq * rows, n_near * n_chan), BF16),
                dma((GROUPS + 1,)), dma((n_layers, 3)), dma((2,)), dma((2,)), pltpu.SemaphoreType.REGULAR((max(n_dev // ROW - 1, 1),)), *[dma((GROUPS,)) for _ in range(4)],
            ],
            compiler_params=pltpu.CompilerParams(collective_id=0, has_side_effects=True, vmem_limit_bytes=52 * 2 ** 20),
            name='dilated_stack',
        )(x, w_in, w_res, w_skip)
        return pl.pallas_call(
            assemble_kernel,
            out_shape=(jax.ShapeDtypeStruct((n_seq, rows, n_chan), F32), jax.ShapeDtypeStruct((n_seq, rows, n_skip), F32)),
            in_specs=[pl.BlockSpec(memory_space=pltpu.VMEM)] * 2,
            out_specs=[any_spec] * 2,
            scratch_shapes=[pltpu.VMEM((n_seq, rows, n_chan), F32), pltpu.VMEM((n_seq, rows, n_skip), F32), dma((2, n_seq))],
            compiler_params=pltpu.CompilerParams(vmem_limit_bytes=4 * 2 ** 20),
            name='assemble',
        )(home, skip)

    return jax.shard_map(local_stack, mesh=mesh, in_specs=(act_spec, P(), P(), P()), out_specs=(act_spec, act_spec), check_vma=False)
```

```python
import functools

import jax
import jax.numpy as jnp
from jax import lax
from jax.experimental import pallas as pl
from jax.experimental.pallas import tpu as pltpu
from jax.sharding import PartitionSpec as P

MESH = pl.DeviceIdType.MESH
F32, BF16 = jnp.float32, jnp.bfloat16
TILE = 8
AHEAD = 3
UNROLL = 31
ROW = 8
HALO = 16
EDGE = 24
GROUPS = 2
COLS = 256


def swap_halves(first, second):
    half = first.shape[1] // 2
    upper = lax.broadcasted_iota(jnp.int32, first.shape, 1) < half
    return jnp.where(upper, first, pltpu.roll(second, half, 1)), jnp.where(upper, pltpu.roll(first, half, 1), second)


def stack_kernel(n_dev, n_near, xv, win_hbm, wres_hbm, wskip_hbm, home, skip_out, win, wres, wskip, halo_l, halo_r,
                 near, near_skip, mid_out, mid_in, far, far_skip, end_out, lhs, gate, near_gate,
                 own_sem, w_sem, halo_send, halo_recv, ready_sem, mid_send, mid_recv, end_send, end_recv):
    me = lax.axis_index('sp')
    n_seq, rows, n_chan = xv.shape
    n_skip = far_skip.shape[2]
    n_layers = win.shape[0]
    far_rows = far_skip.shape[1]
    pad = (far.shape[1] - far_rows) // 2
    in_group = n_seq // GROUPS
    n_res = n_dev // in_group
    part = rows // n_res
    lanes = n_chan * part // TILE
    n_side = TILE // part
    last = n_dev - 1

    def weight_copies(layer):
        return [pltpu.make_async_copy(win_hbm.at[layer], win.at[layer], w_sem.at[layer, 0]),
                pltpu.make_async_copy(wres_hbm.at[layer], wres.at[layer], w_sem.at[layer, 1]),
                pltpu.make_async_copy(wskip_hbm.at[layer], wskip.at[layer], w_sem.at[layer, 2])]

    def start_weights(*layers):
        for layer in layers:
            for copy in weight_copies(layer):
                copy.start()

    start_weights(0)

    n_rows = n_dev // ROW
    row, col = me // ROW, lax.rem(me, ROW)
    barrier = pltpu.get_barrier_semaphore()

    def tell(sem, dst):
        pl.semaphore_signal(sem, inc=1, device_id={'sp': dst}, device_id_type=MESH)

    for k in range(1, ROW):
        tell(barrier, row * ROW + lax.rem(col + k, ROW))

    up, down = row > 0, row < n_rows - 1

    def tell_column(sem):
        @pl.when(up)
        def _():
            tell(sem, me - ROW)

        @pl.when(down)
        def _():
            tell(sem, me + ROW)

    tell_column(barrier)
    before, after = jnp.logical_and(col == 0, up), jnp.logical_and(col == ROW - 1, down)

    @pl.when(before)
    def _():
        tell(barrier, me - 1)

    @pl.when(after)
    def _():
        tell(barrier, me + 1)

    def count(*conditions):
        return sum(jnp.where(c, 1, 0) for c in conditions)

    def heard_column(step):
        pl.semaphore_wait(ready_sem.at[step - 1], count(up, down))
        if step < n_rows - 1:
            tell_column(ready_sem.at[step])

    zero_edge = jnp.zeros((n_seq, EDGE, n_chan), F32)
    near[:, :EDGE] = zero_edge
    near[:, EDGE + rows:] = zero_edge
    for group in range(GROUPS):
        far[group, :pad] = jnp.zeros((pad, n_chan), F32)
        far[group, pad + far_rows:] = jnp.zeros((pad, n_chan), F32)

    pl.semaphore_wait(barrier, ROW - 1 + count(up, down, before, after))
    tell_column(ready_sem.at[0])
    start_weights(*range(1, n_near - 1))


    def seqs_of(group):
        return pl.ds(group * in_group, in_group)

    def to_next(group):
        return pltpu.make_async_remote_copy(src_ref=xv.at[seqs_of(group), pl.ds(rows - HALO, HALO)], dst_ref=halo_l.at[seqs_of(group)],
                                            send_sem=halo_send.at[0, group], recv_sem=halo_recv.at[0, group],
                                            device_id={'sp': me + 1}, device_id_type=MESH)

    def to_prev(group):
        return pltpu.make_async_remote_copy(src_ref=xv.at[seqs_of(group), pl.ds(0, HALO)], dst_ref=halo_r.at[seqs_of(group)],
                                            send_sem=halo_send.at[1, group], recv_sem=halo_recv.at[1, group],
                                            device_id={'sp': me - 1}, device_id_type=MESH)

    for group in range(GROUPS):
        @pl.when(me < last)
        def _():
            to_next(group).start()

        @pl.when(me > 0)
        def _():
            to_prev(group).start()

    near[:, EDGE:EDGE + rows] = xv[...].astype(F32)
    if n_rows > 1:
        heard_column(1)

    def take_halo(group):
        every = slice(group * in_group, (group + 1) * in_group)

        @pl.when(me > 0)
        def _():
            to_next(group).wait_recv()
            near[every, EDGE - HALO:EDGE] = halo_l[every].astype(F32)

        @pl.when(me < last)
        def _():
            to_prev(group).wait_recv()
            near[every, EDGE + rows:EDGE + rows + HALO] = halo_r[every].astype(F32)

    def gated_layer(layer, m):
        w = win.at[layer]
        for col in range(0, n_chan, COLS):
            f = jnp.zeros((m, COLS), F32)
            g = jnp.zeros((m, COLS), F32)
            for tap in range(3):
                op = lhs[:m, tap * n_chan:(tap + 1) * n_chan]
                f = f + jnp.dot(op, w[tap, :, col:col + COLS], preferred_element_type=F32)
                g = g + jnp.dot(op, w[tap, :, n_chan + col:n_chan + col + COLS], preferred_element_type=F32)
            gate[:m, col:col + COLS] = (jnp.tanh(f) * (0.5 * jnp.tanh(0.5 * g) + 0.5)).astype(BF16)

    def near_phase(group):
        seqs = range(group * in_group, (group + 1) * in_group)
        every = slice(group * in_group, (group + 1) * in_group)
        for layer in range(n_near):
            dist = 2 ** layer
            reach = -(-(2 ** n_near - 2 * dist) // TILE) * TILE
            lo, hi = EDGE - reach, EDGE + rows + reach
            size = hi - lo
            m = in_group * size
            for tap in range(3):
                off = lo + (tap - 1) * dist
                for at, seq in enumerate(seqs):
                    lhs[at * size:(at + 1) * size, tap * n_chan:(tap + 1) * n_chan] = near[seq, off:off + size].astype(BF16)
            if group == 0:
                for copy in weight_copies(layer):
                    copy.wait()
                if layer == 1:
                    start_weights(*range(n_near, n_near + AHEAD))
                if layer == n_near - 1:
                    start_weights(*range(n_near + AHEAD, n_layers))
            gated_layer(layer, m)
            for at, seq in enumerate(seqs):
                begin = at * size + EDGE - lo
                near_gate[seq * rows:(seq + 1) * rows, layer * n_chan:(layer + 1) * n_chan] = gate[begin:begin + rows]
            for col in range(0, n_chan, COLS):
                res = jnp.dot(gate[:m], wres[layer, :, col:col + COLS], preferred_element_type=F32).reshape(in_group, size, COLS)
                near[every, lo:hi, col:col + COLS] = near[every, lo:hi, col:col + COLS] + res
            if group == 0 and layer + 2 < n_rows:
                heard_column(layer + 2)
            if layer < n_near - 1:
                @pl.when(me == 0)
                def _():
                    near[every, :EDGE] = zero_edge[:in_group]

                @pl.when(me == last)
                def _():
                    near[every, EDGE + rows:] = zero_edge[:in_group]

        for at, seq in enumerate(seqs):
            for low in range(0, n_res, TILE):
                sides = [near[seq, EDGE:EDGE + rows, side * lanes:(side + 1) * lanes].reshape(part, n_res, lanes)[:, low:low + TILE]
                         for side in range(n_side)]
                mid_out[group, at * n_res + low:at * n_res + low + TILE] = jnp.swapaxes(jnp.concatenate(sides, axis=0), 0, 1)

    def mid_copy(group, dst):
        return pltpu.make_async_remote_copy(src_ref=mid_out.at[group, dst], dst_ref=mid_in.at[group, me], send_sem=mid_send.at[group],
                                            recv_sem=mid_recv.at[group], device_id={'sp': dst}, device_id_type=MESH)

    def send_mid(group):
        @pl.loop(1, n_dev, unroll=UNROLL)
        def _(k):
            mid_copy(group, lax.rem(me + k, n_dev)).start()

        mid_in[group, me] = mid_out[group, me]

    for group in range(GROUPS):
        take_halo(group)
        if group == 0:
            start_weights(n_near - 1)
        near_phase(group)
        if group == 0:
            for step in range(n_near + 2, n_rows):
                heard_column(step)
        send_mid(group)

    def end_copy(group, dst):
        return pltpu.make_async_remote_copy(src_ref=end_out.at[group, dst // 2, lax.rem(dst, 2)], dst_ref=home.at[group, me],
                                            send_sem=end_send.at[group], recv_sem=end_recv.at[group], device_id={'sp': dst}, device_id_type=MESH)

    def own_copy(group):
        return pltpu.make_async_copy(end_out.at[group, me // 2, lax.rem(me, 2)], home.at[group, me], own_sem.at[group])

    def send_home(group):
        if group == 0:
            @pl.loop(1, n_dev, unroll=UNROLL)
            def _(k):
                end_copy(group, lax.rem(me + k, n_dev)).start()

        else:
            skipped = me + 1 - 2 * lax.rem(me, 2)

            @pl.loop(0, n_dev - 1, unroll=UNROLL)
            def _(k):
                place = k + jnp.where(k >= skipped, 1, 0)
                end_copy(group, place + 1 - 2 * lax.rem(place, 2)).start()

        own_copy(group).start()

    others = pl.ds(0, n_dev - 1)

    def wait_all(ref, sem):
        pltpu.make_async_copy(ref.at[others], ref.at[others], sem).wait()

    for layer in range(n_near, n_layers):
        for copy in weight_copies(layer):
            copy.wait()

    for group in range(GROUPS):
        wait_all(mid_in.at[group], mid_recv.at[group])
        blocks = mid_in[group].reshape(n_dev // 2, 2, TILE, lanes)
        for side, value in enumerate(swap_halves(blocks[:, 0], blocks[:, 1])):
            far[group, pad:pad + far_rows, side * lanes:(side + 1) * lanes] = value.reshape(far_rows, lanes)
        for layer in range(n_near, n_layers):
            dist = 2 ** layer // n_res
            for tap in range(3):
                off = pad + (tap - 1) * dist
                lhs[:far_rows, tap * n_chan:(tap + 1) * n_chan] = far[group, off:off + far_rows].astype(BF16)
            gated_layer(layer, far_rows)
            for col in range(0, n_chan, COLS):
                res = jnp.dot(gate[:far_rows], wres[layer, :, col:col + COLS], preferred_element_type=F32)
                far[group, pad:pad + far_rows, col:col + COLS] = far[group, pad:pad + far_rows, col:col + COLS] + res
            for col in range(0, n_skip, COLS):
                skip = jnp.dot(gate[:far_rows], wskip[layer, :, col:col + COLS], preferred_element_type=F32)
                if layer > n_near:
                    skip = far_skip[group, :, col:col + COLS] + skip
                far_skip[group, :, col:col + COLS] = skip
        for which, value in enumerate((far[group, pad:pad + far_rows], far_skip[group])):
            sides = [value[:, side * lanes:(side + 1) * lanes].reshape(n_dev // 2, TILE, lanes) for side in range(n_side)]
            for at, block in enumerate(swap_halves(*sides)):
                end_out[group, :, at, which * TILE:(which + 1) * TILE] = block
        send_home(group)

    for col in range(0, n_skip, COLS):
        skip = jnp.zeros((n_seq * rows, COLS), F32)
        for layer in range(n_near):
            skip = skip + jnp.dot(near_gate[:, layer * n_chan:(layer + 1) * n_chan], wskip[layer, :, col:col + COLS], preferred_element_type=F32)
        near_skip[:, :, col:col + COLS] = skip.reshape(n_seq, rows, COLS)
    skip_copy = pltpu.make_async_copy(near_skip, skip_out, own_sem.at[GROUPS])
    skip_copy.start()

    for group in range(GROUPS):
        wait_all(mid_out.at[group], mid_send.at[group])
    for group in range(GROUPS):
        wait_all(home.at[group], end_recv.at[group])
    for group in range(GROUPS):
        wait_all(home.at[group], end_send.at[group])
        own_copy(group).wait()
    skip_copy.wait()

    for group in range(GROUPS):
        @pl.when(me < last)
        def _():
            to_next(group).wait_send()

        @pl.when(me > 0)
        def _():
            to_prev(group).wait_send()


def assemble_kernel(home, skip, h_out, s_out, h_rows, s_rows, sems):
    n_seq, rows, n_chan = h_rows.shape
    lanes = home.shape[3]
    in_group = n_seq // GROUPS
    n_res = home.shape[1] // in_group
    part = rows // n_res

    def copies(seq):
        return (pltpu.make_async_copy(h_rows.at[seq], h_out.at[seq], sems.at[0, seq]),
                pltpu.make_async_copy(s_rows.at[seq], s_out.at[seq], sems.at[1, seq]))

    for seq in range(n_seq):
        group, at = seq // in_group, seq % in_group
        for which, out in enumerate((h_rows, s_rows)):
            for low in range(0, n_res, TILE):
                blocks = home[group, at * n_res + low:at * n_res + low + TILE, which * TILE:(which + 1) * TILE]
                turned = jnp.swapaxes(blocks, 0, 1)
                for k in range(TILE):
                    begin, side = k % part * n_res + low, k // part
                    value = turned[k]
                    if which == 1:
                        value = value + skip[seq, begin:begin + TILE, side * lanes:(side + 1) * lanes]
                    out[seq, begin:begin + TILE, side * lanes:(side + 1) * lanes] = value
            copies(seq)[which].start()
    for seq in range(n_seq):
        for copy in copies(seq):
            copy.wait()


def solution(mesh):
    n_dev = mesh.shape['sp']
    act_spec = P('dp', 'sp', None)

    def local_stack(x, w_in, w_res, w_skip):
        n_seq, rows, n_chan = x.shape
        n_layers, n_skip = w_in.shape[0], w_skip.shape[2]
        n_res = n_dev * GROUPS // n_seq
        n_near = n_res.bit_length() - 1
        far_rows = n_dev * rows // n_res
        pad = 2 ** (n_layers - 1) // n_res
        part = rows // n_res
        lanes = n_chan * part // TILE
        assert TILE == 2 * part and n_skip == n_chan
        any_spec = pl.BlockSpec(memory_space=pl.ANY)
        m_max = n_seq // GROUPS * (rows + 2 * HALO)
        dma = pltpu.SemaphoreType.DMA
        home, skip = pl.pallas_call(
            functools.partial(stack_kernel, n_dev, n_near),
            out_shape=(jax.ShapeDtypeStruct((GROUPS, n_dev, 2 * TILE, lanes), F32), jax.ShapeDtypeStruct((n_seq, rows, n_skip), F32)),
            in_specs=[pl.BlockSpec(memory_space=pltpu.VMEM)] + [any_spec] * 3,
            out_specs=[any_spec] * 2,
            scratch_shapes=[
                pltpu.VMEM(w_in.shape, BF16), pltpu.VMEM(w_res.shape, BF16), pltpu.VMEM(w_skip.shape, BF16),
                pltpu.VMEM((n_seq, HALO, n_chan), BF16), pltpu.VMEM((n_seq, HALO, n_chan), BF16),
                pltpu.VMEM((n_seq, rows + 2 * EDGE, n_chan), F32), pltpu.VMEM((n_seq, rows, n_skip), F32),
                pltpu.VMEM((GROUPS, n_dev, TILE, lanes), F32), pltpu.VMEM((GROUPS, n_dev, TILE, lanes), F32),
                pltpu.VMEM((GROUPS, far_rows + 2 * pad, n_chan), F32), pltpu.VMEM((GROUPS, far_rows, n_skip), F32),
                pltpu.VMEM((GROUPS, n_dev // 2, 2, 2 * TILE, lanes), F32),
                pltpu.VMEM((m_max, 3 * n_chan), BF16), pltpu.VMEM((m_max, n_chan), BF16), pltpu.VMEM((n_seq * rows, n_near * n_chan), BF16),
                dma((GROUPS + 1,)), dma((n_layers, 3)), dma((2, GROUPS)), dma((2, GROUPS)), pltpu.SemaphoreType.REGULAR((max(n_dev // ROW - 1, 1),)), *[dma((GROUPS,)) for _ in range(4)],
            ],
            compiler_params=pltpu.CompilerParams(collective_id=0, has_side_effects=True, vmem_limit_bytes=52 * 2 ** 20),
            name='dilated_stack',
        )(x, w_in, w_res, w_skip)
        return pl.pallas_call(
            assemble_kernel,
            out_shape=(jax.ShapeDtypeStruct((n_seq, rows, n_chan), F32), jax.ShapeDtypeStruct((n_seq, rows, n_skip), F32)),
            in_specs=[pl.BlockSpec(memory_space=pltpu.VMEM)] * 2,
            out_specs=[any_spec] * 2,
            scratch_shapes=[pltpu.VMEM((n_seq, rows, n_chan), F32), pltpu.VMEM((n_seq, rows, n_skip), F32), dma((2, n_seq))],
            compiler_params=pltpu.CompilerParams(vmem_limit_bytes=4 * 2 ** 20),
            name='assemble',
        )(home, skip)

    return jax.shard_map(local_stack, mesh=mesh, in_specs=(act_spec, P(), P(), P()), out_specs=(act_spec, act_spec), check_vma=False)
```

```python
import functools

import jax
import jax.numpy as jnp
from jax import lax
from jax.experimental import pallas as pl
from jax.experimental.pallas import tpu as pltpu
from jax.sharding import PartitionSpec as P

MESH = pl.DeviceIdType.MESH
F32, BF16 = jnp.float32, jnp.bfloat16
TILE = 8
AHEAD = 3
UNROLL = 31
ROW = 8
HALO = 16
EDGE = 24
GROUPS = 2
COLS = 256


def swap_halves(first, second):
    half = first.shape[1] // 2
    upper = lax.broadcasted_iota(jnp.int32, first.shape, 1) < half
    return jnp.where(upper, first, pltpu.roll(second, half, 1)), jnp.where(upper, pltpu.roll(first, half, 1), second)


def stack_kernel(n_dev, n_near, xv, win_hbm, wres_hbm, wskip_hbm, home, skip_out, win, wres, wskip, halo_l, halo_r,
                 near, near_skip, mid_out, mid_in, far, far_skip, end_out, lhs, gate, near_gate,
                 own_sem, w_sem, halo_send, halo_recv, ready_sem, mid_send, mid_recv, end_send, end_recv):
    me = lax.axis_index('sp')
    n_seq, rows, n_chan = xv.shape
    n_skip = far_skip.shape[2]
    n_layers = win.shape[0]
    far_rows = far_skip.shape[1]
    pad = (far.shape[1] - far_rows) // 2
    in_group = n_seq // GROUPS
    n_res = n_dev // in_group
    part = rows // n_res
    lanes = n_chan * part // TILE
    n_side = TILE // part
    last = n_dev - 1

    def weight_copies(layer):
        return [pltpu.make_async_copy(win_hbm.at[layer], win.at[layer], w_sem.at[layer, 0]),
                pltpu.make_async_copy(wres_hbm.at[layer], wres.at[layer], w_sem.at[layer, 1]),
                pltpu.make_async_copy(wskip_hbm.at[layer], wskip.at[layer], w_sem.at[layer, 2])]

    def start_weights(*layers):
        for layer in layers:
            for copy in weight_copies(layer):
                copy.start()

    start_weights(0)

    n_rows = n_dev // ROW
    row, col = me // ROW, lax.rem(me, ROW)
    barrier = pltpu.get_barrier_semaphore()

    def tell(sem, dst):
        pl.semaphore_signal(sem, inc=1, device_id={'sp': dst}, device_id_type=MESH)

    for k in range(1, ROW):
        tell(barrier, row * ROW + lax.rem(col + k, ROW))

    up, down = row > 0, row < n_rows - 1

    def tell_column(sem):
        @pl.when(up)
        def _():
            tell(sem, me - ROW)

        @pl.when(down)
        def _():
            tell(sem, me + ROW)

    tell_column(barrier)
    before, after = jnp.logical_and(col == 0, up), jnp.logical_and(col == ROW - 1, down)

    @pl.when(before)
    def _():
        tell(barrier, me - 1)

    @pl.when(after)
    def _():
        tell(barrier, me + 1)

    def count(*conditions):
        return sum(jnp.where(c, 1, 0) for c in conditions)

    def heard_column(step):
        pl.semaphore_wait(ready_sem.at[step - 1], count(up, down))
        if step < n_rows - 1:
            tell_column(ready_sem.at[step])

    zero_edge = jnp.zeros((n_seq, EDGE, n_chan), F32)
    near[:, :EDGE] = zero_edge
    near[:, EDGE + rows:] = zero_edge
    for group in range(GROUPS):
        far[group, :pad] = jnp.zeros((pad, n_chan), F32)
        far[group, pad + far_rows:] = jnp.zeros((pad, n_chan), F32)

    pl.semaphore_wait(barrier, ROW - 1 + count(up, down, before, after))
    tell_column(ready_sem.at[0])
    start_weights(*range(1, n_near - 1))


    def seqs_of(group):
        return pl.ds(group * in_group, in_group)

    def to_next(group):
        return pltpu.make_async_remote_copy(src_ref=xv.at[seqs_of(group), pl.ds(rows - HALO, HALO)], dst_ref=halo_l.at[seqs_of(group)],
                                            send_sem=halo_send.at[0, group], recv_sem=halo_recv.at[0, group],
                                            device_id={'sp': me + 1}, device_id_type=MESH)

    def to_prev(group):
        return pltpu.make_async_remote_copy(src_ref=xv.at[seqs_of(group), pl.ds(0, HALO)], dst_ref=halo_r.at[seqs_of(group)],
                                            send_sem=halo_send.at[1, group], recv_sem=halo_recv.at[1, group],
                                            device_id={'sp': me - 1}, device_id_type=MESH)

    for group in range(GROUPS):
        @pl.when(me < last)
        def _():
            to_next(group).start()

        @pl.when(me > 0)
        def _():
            to_prev(group).start()

    near[:, EDGE:EDGE + rows] = xv[...].astype(F32)
    if n_rows > 1:
        heard_column(1)

    def take_halo(group):
        every = slice(group * in_group, (group + 1) * in_group)

        @pl.when(me > 0)
        def _():
            to_next(group).wait_recv()
            near[every, EDGE - HALO:EDGE] = halo_l[every].astype(F32)

        @pl.when(me < last)
        def _():
            to_prev(group).wait_recv()
            near[every, EDGE + rows:EDGE + rows + HALO] = halo_r[every].astype(F32)

    def gated_layer(layer, m):
        w = win.at[layer]
        for col in range(0, n_chan, COLS):
            f = jnp.zeros((m, COLS), F32)
            g = jnp.zeros((m, COLS), F32)
            for tap in range(3):
                op = lhs[:m, tap * n_chan:(tap + 1) * n_chan]
                f = f + jnp.dot(op, w[tap, :, col:col + COLS], preferred_element_type=F32)
                g = g + jnp.dot(op, w[tap, :, n_chan + col:n_chan + col + COLS], preferred_element_type=F32)
            gate[:m, col:col + COLS] = (jnp.tanh(f) * (0.5 * jnp.tanh(0.5 * g) + 0.5)).astype(BF16)

    def near_phase(group):
        seqs = range(group * in_group, (group + 1) * in_group)
        every = slice(group * in_group, (group + 1) * in_group)
        for layer in range(n_near):
            dist = 2 ** layer
            reach = -(-(2 ** n_near - 2 * dist) // TILE) * TILE
            lo, hi = EDGE - reach, EDGE + rows + reach
            size = hi - lo
            m = in_group * size
            for tap in range(3):
                off = lo + (tap - 1) * dist
                for at, seq in enumerate(seqs):
                    lhs[at * size:(at + 1) * size, tap * n_chan:(tap + 1) * n_chan] = near[seq, off:off + size].astype(BF16)
            if group == 0:
                for copy in weight_copies(layer):
                    copy.wait()
                if layer == 1:
                    start_weights(*range(n_near, n_near + AHEAD))
                if layer == n_near - 1:
                    start_weights(*range(n_near + AHEAD, n_layers))
            gated_layer(layer, m)
            for at, seq in enumerate(seqs):
                begin = at * size + EDGE - lo
                near_gate[seq * rows:(seq + 1) * rows, layer * n_chan:(layer + 1) * n_chan] = gate[begin:begin + rows]
            for col in range(0, n_chan, COLS):
                res = jnp.dot(gate[:m], wres[layer, :, col:col + COLS], preferred_element_type=F32).reshape(in_group, size, COLS)
                near[every, lo:hi, col:col + COLS] = near[every, lo:hi, col:col + COLS] + res
            if group == 0 and layer + 2 < n_rows:
                heard_column(layer + 2)
            if layer < n_near - 1:
                @pl.when(me == 0)
                def _():
                    near[every, :EDGE] = zero_edge[:in_group]

                @pl.when(me == last)
                def _():
                    near[every, EDGE + rows:] = zero_edge[:in_group]

        for at, seq in enumerate(seqs):
            for low in range(0, n_res, TILE):
                sides = [near[seq, EDGE:EDGE + rows, side * lanes:(side + 1) * lanes].reshape(part, n_res, lanes)[:, low:low + TILE]
                         for side in range(n_side)]
                mid_out[group, at * n_res + low:at * n_res + low + TILE] = jnp.swapaxes(jnp.concatenate(sides, axis=0), 0, 1)

    def mid_copy(group, dst):
        return pltpu.make_async_remote_copy(src_ref=mid_out.at[group, dst], dst_ref=mid_in.at[group, me], send_sem=mid_send.at[group],
                                            recv_sem=mid_recv.at[group], device_id={'sp': dst}, device_id_type=MESH)

    def send_mid(group):
        @pl.loop(1, n_dev, unroll=UNROLL)
        def _(k):
            mid_copy(group, lax.rem(me + n_dev - k, n_dev)).start()

        mid_in[group, me] = mid_out[group, me]

    for group in range(GROUPS):
        take_halo(group)
        if group == 0:
            start_weights(n_near - 1)
        near_phase(group)
        if group == 0:
            for step in range(n_near + 2, n_rows):
                heard_column(step)
        send_mid(group)

    def end_copy(group, dst):
        return pltpu.make_async_remote_copy(src_ref=end_out.at[group, dst // 2, lax.rem(dst, 2)], dst_ref=home.at[group, me],
                                            send_sem=end_send.at[group], recv_sem=end_recv.at[group], device_id={'sp': dst}, device_id_type=MESH)

    def own_copy(group):
        return pltpu.make_async_copy(end_out.at[group, me // 2, lax.rem(me, 2)], home.at[group, me], own_sem.at[group])

    def send_home(group):
        if group == 0:
            @pl.loop(1, n_dev, unroll=UNROLL)
            def _(k):
                end_copy(group, lax.rem(me + k, n_dev)).start()

        else:
            skipped = me + 1 - 2 * lax.rem(me, 2)

            @pl.loop(0, n_dev - 1, unroll=UNROLL)
            def _(k):
                place = k + jnp.where(k >= skipped, 1, 0)
                end_copy(group, place + 1 - 2 * lax.rem(place, 2)).start()

        own_copy(group).start()

    others = pl.ds(0, n_dev - 1)

    def wait_all(ref, sem):
        pltpu.make_async_copy(ref.at[others], ref.at[others], sem).wait()

    for layer in range(n_near, n_layers):
        for copy in weight_copies(layer):
            copy.wait()

    for group in range(GROUPS):
        wait_all(mid_in.at[group], mid_recv.at[group])
        blocks = mid_in[group].reshape(n_dev // 2, 2, TILE, lanes)
        for side, value in enumerate(swap_halves(blocks[:, 0], blocks[:, 1])):
            far[group, pad:pad + far_rows, side * lanes:(side + 1) * lanes] = value.reshape(far_rows, lanes)
        for layer in range(n_near, n_layers):
            dist = 2 ** layer // n_res
            for tap in range(3):
                off = pad + (tap - 1) * dist
                lhs[:far_rows, tap * n_chan:(tap + 1) * n_chan] = far[group, off:off + far_rows].astype(BF16)
            gated_layer(layer, far_rows)
            for col in range(0, n_chan, COLS):
                res = jnp.dot(gate[:far_rows], wres[layer, :, col:col + COLS], preferred_element_type=F32)
                far[group, pad:pad + far_rows, col:col + COLS] = far[group, pad:pad + far_rows, col:col + COLS] + res
            for col in range(0, n_skip, COLS):
                skip = jnp.dot(gate[:far_rows], wskip[layer, :, col:col + COLS], preferred_element_type=F32)
                if layer > n_near:
                    skip = far_skip[group, :, col:col + COLS] + skip
                far_skip[group, :, col:col + COLS] = skip
        for which, value in enumerate((far[group, pad:pad + far_rows], far_skip[group])):
            sides = [value[:, side * lanes:(side + 1) * lanes].reshape(n_dev // 2, TILE, lanes) for side in range(n_side)]
            for at, block in enumerate(swap_halves(*sides)):
                end_out[group, :, at, which * TILE:(which + 1) * TILE] = block
        send_home(group)

    for col in range(0, n_skip, COLS):
        skip = jnp.zeros((n_seq * rows, COLS), F32)
        for layer in range(n_near):
            skip = skip + jnp.dot(near_gate[:, layer * n_chan:(layer + 1) * n_chan], wskip[layer, :, col:col + COLS], preferred_element_type=F32)
        near_skip[:, :, col:col + COLS] = skip.reshape(n_seq, rows, COLS)
    skip_copy = pltpu.make_async_copy(near_skip, skip_out, own_sem.at[GROUPS])
    skip_copy.start()

    for group in range(GROUPS):
        wait_all(mid_out.at[group], mid_send.at[group])
    for group in range(GROUPS):
        wait_all(home.at[group], end_recv.at[group])
    for group in range(GROUPS):
        wait_all(home.at[group], end_send.at[group])
        own_copy(group).wait()
    skip_copy.wait()

    for group in range(GROUPS):
        @pl.when(me < last)
        def _():
            to_next(group).wait_send()

        @pl.when(me > 0)
        def _():
            to_prev(group).wait_send()


def assemble_kernel(home, skip, h_out, s_out, h_rows, s_rows, sems):
    n_seq, rows, n_chan = h_rows.shape
    lanes = home.shape[3]
    in_group = n_seq // GROUPS
    n_res = home.shape[1] // in_group
    part = rows // n_res

    def copies(seq):
        return (pltpu.make_async_copy(h_rows.at[seq], h_out.at[seq], sems.at[0, seq]),
                pltpu.make_async_copy(s_rows.at[seq], s_out.at[seq], sems.at[1, seq]))

    for seq in range(n_seq):
        group, at = seq // in_group, seq % in_group
        for which, out in enumerate((h_rows, s_rows)):
            for low in range(0, n_res, TILE):
                blocks = home[group, at * n_res + low:at * n_res + low + TILE, which * TILE:(which + 1) * TILE]
                turned = jnp.swapaxes(blocks, 0, 1)
                for k in range(TILE):
                    begin, side = k % part * n_res + low, k // part
                    value = turned[k]
                    if which == 1:
                        value = value + skip[seq, begin:begin + TILE, side * lanes:(side + 1) * lanes]
                    out[seq, begin:begin + TILE, side * lanes:(side + 1) * lanes] = value
            copies(seq)[which].start()
    for seq in range(n_seq):
        for copy in copies(seq):
            copy.wait()


def solution(mesh):
    n_dev = mesh.shape['sp']
    act_spec = P('dp', 'sp', None)

    def local_stack(x, w_in, w_res, w_skip):
        n_seq, rows, n_chan = x.shape
        n_layers, n_skip = w_in.shape[0], w_skip.shape[2]
        n_res = n_dev * GROUPS // n_seq
        n_near = n_res.bit_length() - 1
        far_rows = n_dev * rows // n_res
        pad = 2 ** (n_layers - 1) // n_res
        part = rows // n_res
        lanes = n_chan * part // TILE
        assert TILE == 2 * part and n_skip == n_chan
        any_spec = pl.BlockSpec(memory_space=pl.ANY)
        m_max = n_seq // GROUPS * (rows + 2 * HALO)
        dma = pltpu.SemaphoreType.DMA
        home, skip = pl.pallas_call(
            functools.partial(stack_kernel, n_dev, n_near),
            out_shape=(jax.ShapeDtypeStruct((GROUPS, n_dev, 2 * TILE, lanes), F32), jax.ShapeDtypeStruct((n_seq, rows, n_skip), F32)),
            in_specs=[pl.BlockSpec(memory_space=pltpu.VMEM)] + [any_spec] * 3,
            out_specs=[any_spec] * 2,
            scratch_shapes=[
                pltpu.VMEM(w_in.shape, BF16), pltpu.VMEM(w_res.shape, BF16), pltpu.VMEM(w_skip.shape, BF16),
                pltpu.VMEM((n_seq, HALO, n_chan), BF16), pltpu.VMEM((n_seq, HALO, n_chan), BF16),
                pltpu.VMEM((n_seq, rows + 2 * EDGE, n_chan), F32), pltpu.VMEM((n_seq, rows, n_skip), F32),
                pltpu.VMEM((GROUPS, n_dev, TILE, lanes), F32), pltpu.VMEM((GROUPS, n_dev, TILE, lanes), F32),
                pltpu.VMEM((GROUPS, far_rows + 2 * pad, n_chan), F32), pltpu.VMEM((GROUPS, far_rows, n_skip), F32),
                pltpu.VMEM((GROUPS, n_dev // 2, 2, 2 * TILE, lanes), F32),
                pltpu.VMEM((m_max, 3 * n_chan), BF16), pltpu.VMEM((m_max, n_chan), BF16), pltpu.VMEM((n_seq * rows, n_near * n_chan), BF16),
                dma((GROUPS + 1,)), dma((n_layers, 3)), dma((2, GROUPS)), dma((2, GROUPS)), pltpu.SemaphoreType.REGULAR((max(n_dev // ROW - 1, 1),)), *[dma((GROUPS,)) for _ in range(4)],
            ],
            compiler_params=pltpu.CompilerParams(collective_id=0, has_side_effects=True, vmem_limit_bytes=52 * 2 ** 20),
            name='dilated_stack',
        )(x, w_in, w_res, w_skip)
        return pl.pallas_call(
            assemble_kernel,
            out_shape=(jax.ShapeDtypeStruct((n_seq, rows, n_chan), F32), jax.ShapeDtypeStruct((n_seq, rows, n_skip), F32)),
            in_specs=[pl.BlockSpec(memory_space=pltpu.VMEM)] * 2,
            out_specs=[any_spec] * 2,
            scratch_shapes=[pltpu.VMEM((n_seq, rows, n_chan), F32), pltpu.VMEM((n_seq, rows, n_skip), F32), dma((2, n_seq))],
            compiler_params=pltpu.CompilerParams(vmem_limit_bytes=4 * 2 ** 20),
            name='assemble',
        )(home, skip)

    return jax.shard_map(local_stack, mesh=mesh, in_specs=(act_spec, P(), P(), P()), out_specs=(act_spec, act_spec), check_vma=False)
```
